32 devices in a mesh: groups: 2 (over x), ep: 16 (over z, y, core).
Axes of the slice: x: 2, y: 2, z: 4, core: 2. Of those that a mesh axis runs over, the one named last changes fastest.
Arguments:
- tokens: bfloat16 [4096, 3584], P(('groups', 'ep')), parts along dimension 0, may hold values from -6 to 6
- host: int32 [4096, 2], P(('groups', 'ep')), parts along dimension 0, may hold values from 0 to 7, all different within a row; in each aligned block of 128 rows (0 to 127, 128 to 255, ...) at most 40 rows name the same one
- copy: int32 [4096, 2], P(('groups', 'ep')), parts along dimension 0, may hold values from 0 to 1
- gate_prob: float32 [4096, 2], P(('groups', 'ep')), parts along dimension 0, may hold values from 0.1 to 1
- hot: int32 [8], replicated, may hold values from 0 to 7, each once
- w_gate: bfloat16 [16, 1792, 1024], P('ep'), may hold values from -0.09375 to 0.09375
- w_up: bfloat16 [16, 1792, 1024], P('ep'), may hold values from -0.09375 to 0.09375
- w_down: bfloat16 [16, 1024, 1792], P('ep'), may hold values from -0.1875 to 0.1875
- gate_scale: float32 [16, 14, 8], P('ep'), may hold values from 0.3 to 3
- up_scale: float32 [16, 14, 8], P('ep'), may hold values from 0.3 to 3
- down_scale: float32 [16, 8, 14], P('ep'), may hold values from 0.3 to 3
Outputs:
- mixed: bfloat16 [4096, 3584], P(('groups', 'ep')), parts along dimension 0
The draws below stay inside these ranges and needn't reach their ends.
There are 2 independent parts, one for each index of `groups`. The reference program is written for one: setup_inputs(seed, part) draws one part's arguments, and reference() takes and returns one part's arrays. A program takes and returns all parts, laid end to end along the dimension named above; an argument that names none is the same for every part. Nothing has to cross between parts.
Inputs may be any that keep to these rules, and one draw needn't show every extreme that they name: Each row names 2 different host groups; no group is named by more than 40 of the rows of one device. `hot`: A permutation of the 8 experts.
All inputs are finite; a program needn't handle non-finite values.
Results may differ from the reference program's by a relative error of at most 0.0087.
Values may be sent and summed in bfloat16 or wider, within the bound.
A program may use at most 192 MiB of HBM per device.

```python
import math
import jax
import jax.numpy as jnp
import numpy as np
from jax import lax

D = 3584
HIDDEN_SIZE = 1024
BLOCK = 128
SPLIT = 2
TOP = 2
TOK_DEV = 128
EXPERTS = 8
CAP = 40
TOKENS = 2048
N_EP = 16


def touch_ends(array, rng, low, largest):
    shape = array.shape
    index_at = [jax.random.randint(jax.random.fold_in(rng, axis), (), 0, shape[axis]) for axis in range(len(shape))]
    array = array.at[tuple(index_at)].set(low)
    longest = shape.index(max(shape))
    index_at[longest] = (index_at[longest] + 1) % shape[longest]
    return array.at[tuple(index_at)].set(largest)


def steps_of(key, extent, cuts, smallest, largest):
    loudness, own = 1.0, jax.random.fold_in(key, 6)
    for position, parts in cuts:
        steps = jnp.exp(jax.random.uniform(jax.random.fold_in(own, position), (parts,), jnp.float32, smallest / len(cuts), largest / len(cuts)))
        loudness = loudness * jnp.repeat(steps, extent[position] // parts).reshape([-1 if axis == position else 1 for axis in range(len(extent))])
    return loudness


def shared_out(rng, own, number, rows, amount, top, limit, slope):
    sequence = jax.random.permutation(rng, amount)
    packed, common = load_shares(amount, rows * top, limit, slope, True), load_shares(amount, rows * top, limit, slope, False)
    places = jnp.arange(amount)

    def named(tallies, rotation):
        used = int((tallies > 0).sum())
        fixed = max(1, used // 4)
        shifted = fixed + (places - fixed + rotation * (used - fixed)) % max(1, amount - fixed)
        return jnp.zeros((amount,), jnp.int32).at[sequence[jnp.where(places < fixed, places, shifted)]].set(jnp.asarray(tallies, jnp.int32))

    tallies = jnp.where(number % 4 == 0, named(packed, number // 4), named(common, number - number // 4 - 1))
    mixed = jax.random.permutation(jax.random.fold_in(own, 3), amount)
    source_of, sink = mixed[0:amount // 2 * 2:2], mixed[1:amount // 2 * 2:2]
    slack = jnp.minimum(tallies[source_of] - 1, limit - tallies[sink]) // 2
    slack = jnp.where((source_of == sequence[0]) | (sink == sequence[0]) | (tallies[sink] == 0), 0, jnp.maximum(slack, 0))
    shifted = jax.random.randint(jax.random.fold_in(own, 4), (amount // 2,), 0, 1 << 20) % (slack + 1)
    tallies = tallies.at[source_of].add(-shifted).at[sink].add(shifted)
    items = jnp.searchsorted(jnp.cumsum(tallies), jnp.arange(rows * top), side="right").astype(jnp.int32)
    table = items.reshape(top, rows).T
    table = table[jax.random.permutation(jax.random.fold_in(own, 1), rows)]
    rotation = jax.random.randint(jax.random.fold_in(own, 2), (rows, 1), 0, top)
    return jnp.take_along_axis(table, (jnp.arange(top)[None, :] + rotation) % top, axis=1)


def load_shares(number_of, total, limit, skew, full):
    weights = [(1 << 20) // math.isqrt(standing ** skew) + 1 for standing in range(1, number_of + 1)]
    largest = limit if full else min(limit, max(-(-total // number_of), total * weights[0] // sum(weights)))
    least = 1 if total - largest >= number_of - 1 else 0
    counts, spare = [largest] + [least] * (number_of - 1), total - largest - least * (number_of - 1)
    while spare > 0:
        free = [i for i in range(1, number_of) if counts[i] < largest] or [i for i in range(1, number_of) if counts[i] < limit]
        pool, left = sum([weights[i] for i in free]), spare
        for i in free:
            addition = min(limit - counts[i], max(1, left * weights[i] // pool), spare)
            counts[i] = counts[i] + addition
            spare = spare - addition
    return np.array(counts)


def centred(own_key, dims, width, limit, pieces=(), kind=jnp.bfloat16):
    array = jax.random.normal(own_key, dims, jnp.float32) * width
    if len(pieces) > 0:
        array = steps_of(own_key, dims, pieces, -0.22, 0.18) * array
    return jnp.clip(array, min=-limit, max=limit).astype(kind)


def setup_inputs(seed: int = 0, part: int = 0) -> dict:
    splits = jax.random.split(jax.random.key(seed), 12)
    part_keys = jax.random.split(jax.random.fold_in(splits[11], part), 12)
    tokens = centred(part_keys[0], (TOKENS, D), 1.0, 6.0, ((0, 16),))
    host_keys = jax.random.split(jax.random.fold_in(part_keys[1], 1), TOKENS // TOK_DEV)
    host_turns = jax.random.permutation(jax.random.fold_in(part_keys[1], 3), TOKENS // TOK_DEV)
    host = jax.vmap(lambda own, number: shared_out(jax.random.fold_in(part_keys[1], 2), own, number, TOK_DEV, EXPERTS, TOP, CAP, 2))(host_keys, host_turns).reshape((TOKENS, TOP))
    copy = touch_ends(jax.random.randint(part_keys[2], (TOKENS, TOP), 0, 2), jax.random.fold_in(part_keys[2], 1), 0, 1).astype(jnp.int32)
    gate_prob = jnp.clip(jnp.exp(math.log(1.0) - 2.3025851 * jax.random.uniform(part_keys[3], (TOKENS, TOP), jnp.float32) ** steps_of(part_keys[3], (TOKENS, TOP), ((0, 16),), -0.2, 0.2)), 0.1, 1.0)
    hot = jax.random.permutation(splits[4], EXPERTS).astype(jnp.int32)
    w_gate = centred(splits[5], (EXPERTS * SPLIT, D // SPLIT, HIDDEN_SIZE), D ** -0.5, 0.09375, ((0, 16),))
    w_up = centred(splits[6], (EXPERTS * SPLIT, D // SPLIT, HIDDEN_SIZE), D ** -0.5, 0.09375, ((0, 16),))
    w_down = centred(splits[7], (EXPERTS * SPLIT, HIDDEN_SIZE, D // SPLIT), HIDDEN_SIZE ** -0.5, 0.1875, ((0, 16),))
    gate_scale = jnp.clip(jnp.exp(math.log(3.0) - 2.3025851 * jax.random.uniform(splits[8], (EXPERTS * SPLIT, D // SPLIT // BLOCK, HIDDEN_SIZE // BLOCK), jnp.float32) ** steps_of(splits[8], (EXPERTS * SPLIT, D // SPLIT // BLOCK, HIDDEN_SIZE // BLOCK), ((0, 16),), -0.2, 0.2)), 0.3, 3.0)
    up_scale = jnp.clip(jnp.exp(math.log(3.0) - 2.3025851 * jax.random.uniform(splits[9], (EXPERTS * SPLIT, D // SPLIT // BLOCK, HIDDEN_SIZE // BLOCK), jnp.float32) ** steps_of(splits[9], (EXPERTS * SPLIT, D // SPLIT // BLOCK, HIDDEN_SIZE // BLOCK), ((0, 16),), -0.2, 0.2)), 0.3, 3.0)
    down_scale = jnp.clip(jnp.exp(math.log(3.0) - 2.3025851 * jax.random.uniform(splits[10], (EXPERTS * SPLIT, HIDDEN_SIZE // BLOCK, D // SPLIT // BLOCK), jnp.float32) ** steps_of(splits[10], (EXPERTS * SPLIT, HIDDEN_SIZE // BLOCK, D // SPLIT // BLOCK), ((0, 16),), -0.2, 0.2)), 0.3, 3.0)
    return {"tokens": tokens, "host": host, "copy": copy, "gate_prob": gate_prob, "hot": hot, "w_gate": w_gate, "w_up": w_up, "w_down": w_down, "gate_scale": gate_scale, "up_scale": up_scale, "down_scale": down_scale}


def dequant(weight, scales):
    rows_in, cols_in = weight.shape
    row_blocks, col_blocks = scales.shape
    expanded = jnp.repeat(scales, cols_in // col_blocks, axis=1)
    blocks = weight.reshape(row_blocks, rows_in // row_blocks, cols_in).astype(jnp.float32) * expanded[:, None, :]
    return blocks.reshape(rows_in, cols_in).astype(jnp.bfloat16)


def widen(value):
    return lax.optimization_barrier(value.astype(jnp.bfloat16)).astype(jnp.float32)


def reference(tokens, host, copy, gate_prob, hot, w_gate, w_up, w_down, gate_scale, up_scale, down_scale):
    pair_count = TOKENS * TOP
    host_f = host.reshape(pair_count)
    copy_f = copy.reshape(pair_count)
    expert_f = jnp.where(copy_f == 0, host_f, hot[host_f]).astype(jnp.int32)
    weight_f = gate_prob.reshape(pair_count)
    limit_rows = 2 * N_EP * CAP
    half_width = D // SPLIT

    def one_expert(expert, running):
        expert = expert.astype(jnp.int32)
        matches = expert_f == expert
        live_count = jnp.sum(matches.astype(jnp.int32))
        picks = jnp.nonzero(matches, size=limit_rows, fill_value=0)[0].astype(jnp.int32)
        is_valid = (jnp.arange(limit_rows, dtype=jnp.int32) < live_count).astype(jnp.float32)
        chosen = tokens[picks // TOP]
        gate_sum = jnp.zeros((limit_rows, HIDDEN_SIZE), jnp.float32)
        up_sum = jnp.zeros((limit_rows, HIDDEN_SIZE), jnp.float32)
        for part_index in range(SPLIT):
            block_id = expert * SPLIT + part_index
            features = chosen[:, part_index * half_width:(part_index + 1) * half_width]
            gate_mat = dequant(lax.dynamic_index_in_dim(w_gate, block_id, 0, keepdims=False), lax.dynamic_index_in_dim(gate_scale, block_id, 0, keepdims=False))
            up_mat = dequant(lax.dynamic_index_in_dim(w_up, block_id, 0, keepdims=False), lax.dynamic_index_in_dim(up_scale, block_id, 0, keepdims=False))
            gate_sum = gate_sum + widen(jnp.dot(features, gate_mat, preferred_element_type=jnp.float32))
            up_sum = up_sum + widen(jnp.dot(features, up_mat, preferred_element_type=jnp.float32))
        hidden = (jax.nn.silu(gate_sum) * up_sum).astype(jnp.bfloat16)
        halves = []
        for part_index in range(SPLIT):
            block_id = expert * SPLIT + part_index
            down_mat = dequant(lax.dynamic_index_in_dim(w_down, block_id, 0, keepdims=False), lax.dynamic_index_in_dim(down_scale, block_id, 0, keepdims=False))
            halves.append(widen(jnp.dot(hidden, down_mat, preferred_element_type=jnp.float32)))
        expert_out = jnp.concatenate(halves, axis=1)
        contrib = expert_out * (weight_f[picks] * is_valid)[:, None]
        return running.at[picks // TOP].add(contrib)

    running = lax.fori_loop(0, EXPERTS, one_expert, jnp.zeros((TOKENS, D), jnp.float32))
    return running.astype(jnp.bfloat16)
```

```python
import functools

import jax
import jax.numpy as jnp
from jax import lax
from jax.experimental import pallas as pl
from jax.experimental.pallas import tpu as pltpu
from jax.sharding import PartitionSpec as P

SPLIT = 2


def from_partner(value, axis, apart):
    mask = 2**apart
    pairs = [(source, source ^ mask) for source in range(lax.axis_size(axis))]
    return lax.ppermute(value, axis, pairs)


def dequant(weight, scales):
    rows_in, cols_in = weight.shape
    row_blocks, col_blocks = scales.shape
    expanded = jnp.repeat(scales, cols_in // col_blocks, axis=1)
    blocks = (
        weight.reshape(row_blocks, rows_in // row_blocks, cols_in).astype(jnp.float32)
        * expanded[:, None, :]
    )
    return blocks.reshape(rows_in, cols_in).astype(jnp.bfloat16)


def lookup(table_in, keys):
    positions = jnp.arange(table_in.shape[0], dtype=jnp.int32)
    return jnp.sum(jnp.where(keys[:, None] == positions[None, :], table_in[None, :], 0), axis=1)


def padded_exchange(
    tokens, host, copy, gate_prob, hot, w_gate, w_up, w_down, gate_scale, up_scale, down_scale
):
    devices = lax.axis_size("ep")
    experts = devices // SPLIT
    tok_rows, width = tokens.shape
    top_count = host.shape[1]
    capacity = tok_rows * top_count * 5 // (4 * experts)
    half_width = width // SPLIT
    pair_count = tok_rows * top_count
    host_f = host.reshape(pair_count)
    copy_f = copy.reshape(pair_count)
    onehot = (host_f[:, None] == jnp.arange(experts, dtype=jnp.int32)[None, :]).astype(jnp.int32)
    slot_f = jnp.sum((jnp.cumsum(onehot, axis=0) - 1) * onehot, axis=1)
    expert_f = jnp.where(copy_f == 0, host_f, lookup(hot, host_f))
    place_f = copy_f * capacity + slot_f
    tok_split = tokens.reshape(tok_rows, SPLIT, half_width)
    own_gate = dequant(w_gate[0], gate_scale[0])
    own_up = dequant(w_up[0], up_scale[0])
    own_down = dequant(w_down[0], down_scale[0])
    zone_rows = 2 * capacity
    slots_all = experts * zone_rows
    slot_table = (
        jnp.zeros((slots_all,), jnp.int32)
        .at[expert_f * zone_rows + place_f]
        .set(jnp.arange(pair_count, dtype=jnp.int32) + 1)
    )
    slot_table = slot_table.reshape(experts, zone_rows)
    filled = slot_table > 0
    row_of = jnp.maximum(slot_table - 1, 0) // top_count
    picked = tok_split[row_of[:, None, :], jnp.arange(SPLIT, dtype=jnp.int32)[None, :, None]]
    picked = jnp.where(filled[:, None, :, None], picked, jnp.zeros_like(picked))
    outgoing_rows = picked.reshape(devices, zone_rows, half_width)
    received = lax.all_to_all(outgoing_rows, "ep", split_axis=0, concat_axis=0, tiled=True)

    def project(matrix_in, own_mat):
        return jnp.dot(matrix_in, own_mat, preferred_element_type=jnp.float32)

    gate_part = project(received, own_gate).astype(jnp.bfloat16)
    up_part = project(received, own_up).astype(jnp.bfloat16)
    partner_gate, partner_up = from_partner((gate_part, up_part), "ep", 0)
    gate_sum = gate_part.astype(jnp.float32) + partner_gate.astype(jnp.float32)
    up_sum = up_part.astype(jnp.float32) + partner_up.astype(jnp.float32)
    hidden = (jax.nn.silu(gate_sum) * up_sum).astype(jnp.bfloat16)
    results = project(hidden, own_down).astype(jnp.bfloat16)
    returned = lax.all_to_all(results, "ep", split_axis=0, concat_axis=0, tiled=True)
    back_four = returned.reshape(experts, SPLIT, zone_rows, half_width)
    values = back_four[
        expert_f[:, None], jnp.arange(SPLIT, dtype=jnp.int32)[None, :], place_f[:, None]
    ]
    values = values.reshape(tok_rows, top_count, width).astype(jnp.float32)
    mixed = jnp.sum(values * gate_prob[:, :, None], axis=1)
    return mixed.astype(jnp.bfloat16)


def pooled_slots(chip_tokens, top_count, chips):
    mean = chip_tokens * top_count // chips
    return -(-(mean * 13 // 8) // 8) * 8


def offset_of(step, chips):
    return chips // 2 + ((step + 1) // 2) * (1 - 2 * (step % 2))


def fused_kernel(
    chips,
    cores,
    groups,
    slots,
    tokens,
    host,
    copied,
    gate_prob,
    hot,
    w_gate,
    w_up,
    w_down,
    gate_scale,
    up_scale,
    down_scale,
    out,
    flag_out,
    tok_all,
    info_rows,
    info_all,
    gate_mat,
    up_mat,
    down_mat,
    first_rank,
    second_rank,
    send_rows,
    recv_rows,
    part_out,
    part_in,
    hidden_out,
    returned,
    total,
    mixed,
    flag_send,
    flag_recv,
    flag_far,
    local_sem,
    weight_sem,
    pair_send,
    pair_recv,
    row_send,
    row_recv,
    part_send,
    part_recv,
    back_send,
    back_recv,
    flag_ssem,
    flag_rsem,
    far_ssem,
    far_rsem,
):
    rows = tokens.shape[0]
    half = tokens.shape[1] // cores
    hidden_size = gate_mat.shape[1]
    me = lax.axis_index("ep")
    group = lax.axis_index("groups")
    chip = me // cores
    core = me % cores
    other = 1 - core
    partner = {"ep": chip * cores + other}

    def to_chip(offset):
        return {"ep": lax.rem(chip + offset, chips) * cores + core}

    def from_chip(offset):
        return {"ep": lax.rem(chip + chips - offset, chips) * cores + core}

    weight_copies = [
        pltpu.make_async_copy(w_gate.at[0], gate_mat, weight_sem.at[0]),
        pltpu.make_async_copy(w_up.at[0], up_mat, weight_sem.at[1]),
        pltpu.make_async_copy(w_down.at[0], down_mat, weight_sem.at[2]),
    ]
    for copy in weight_copies:
        copy.start()
    my_rows = pl.ds(pl.multiple_of(core * rows, rows), rows)
    your_rows = pl.ds(pl.multiple_of(other * rows, rows), rows)
    my_cols = pl.ds(pl.multiple_of(core * half, 128), half)
    your_cols = pl.ds(pl.multiple_of(other * half, 128), half)
    own_tok = pltpu.make_async_copy(
        tokens.at[:, my_cols], tok_all.at[my_rows, :], local_sem.at[0]
    )
    own_tok.start()
    named = host[...]
    moved = jnp.zeros_like(named)
    for name in range(chips):
        moved = jnp.where(named == name, hot[name], moved)
    expert = jnp.where(copied[...] == 0, named, moved).astype(jnp.float32)
    top_count = named.shape[0]
    info_rows[core] = jnp.concatenate(
        [expert, gate_prob[...], jnp.zeros((8 - 2 * top_count, rows), jnp.float32)], axis=0
    )

    barrier = pltpu.get_barrier_semaphore()
    pl.semaphore_signal(
        barrier, inc=1, device_id=partner, device_id_type=pl.DeviceIdType.MESH
    )
    for far in range(1, groups):
        pl.semaphore_signal(
            barrier,
            inc=1,
            device_id={"groups": lax.rem(group + far, groups)},
            device_id_type=pl.DeviceIdType.MESH,
        )

    @pl.loop(1, chips)
    def _(offset):
        pl.semaphore_signal(
            barrier,
            inc=1,
            device_id=to_chip(offset),
            device_id_type=pl.DeviceIdType.MESH,
        )

    pl.semaphore_wait(barrier, chips + groups - 1)

    def remote(source, target, send, recv, device):
        return pltpu.make_async_remote_copy(
            src_ref=source,
            dst_ref=target,
            send_sem=send,
            recv_sem=recv,
            device_id=device,
            device_id_type=pl.DeviceIdType.MESH,
        )

    pair_info = remote(
        info_rows.at[core], info_rows.at[core], pair_send.at[0], pair_recv.at[0], partner
    )
    pair_tok = remote(
        tokens.at[:, your_cols],
        tok_all.at[my_rows, :],
        pair_send.at[1],
        pair_recv.at[1],
        partner,
    )
    pair_info.start()
    pair_tok.start()
    pair_info.wait()
    for part in range(cores):
        info_all[part * rows : (part + 1) * rows, :] = info_rows[part].T

    pooled = cores * rows
    lanes = lax.broadcasted_iota(jnp.int32, (pooled, 128), 1)
    expert_a = info_all[:, 0:1].astype(jnp.int32)
    expert_b = info_all[:, 1:2].astype(jnp.int32)
    match_a = expert_a == lanes
    match_b = expert_b == lanes
    hot_a = match_a.astype(jnp.float32)
    hot_b = match_b.astype(jnp.float32)
    below = (
        lax.broadcasted_iota(jnp.int32, (pooled, pooled), 1)
        < lax.broadcasted_iota(jnp.int32, (pooled, pooled), 0)
    ).astype(jnp.float32).astype(jnp.bfloat16)
    rank_a = jnp.dot(below, hot_a.astype(jnp.bfloat16), preferred_element_type=jnp.float32)
    rank_b = jnp.dot(below, hot_b.astype(jnp.bfloat16), preferred_element_type=jnp.float32)
    count_a = jnp.sum(hot_a, axis=0, keepdims=True)
    count_b = jnp.sum(hot_b, axis=0, keepdims=True)
    first_rank[...] = jnp.where(match_a, rank_a, -1.0)
    second_rank[...] = jnp.where(match_b, rank_b + count_a, -1.0)
    most = jnp.max(count_a + count_b, axis=1, keepdims=True)
    flag_send[...] = jnp.broadcast_to((most > slots).astype(jnp.float32), flag_send.shape)

    def slot_columns(expert):
        mine = lanes == expert
        column_a = jnp.sum(jnp.where(mine, first_rank[...] + 1.0, 0.0), axis=1, keepdims=True)
        column_b = jnp.sum(jnp.where(mine, second_rank[...] + 1.0, 0.0), axis=1, keepdims=True)
        positions = lax.broadcasted_iota(jnp.int32, (pooled, slots), 1).astype(jnp.float32) + 1.0
        return column_a == positions, column_b == positions

    own_tok.wait()
    pair_tok.wait()

    def pick(offset):
        in_a, in_b = slot_columns(lax.rem(chip + offset, chips))
        chosen = (in_a | in_b).astype(jnp.float32).astype(jnp.bfloat16)
        return lax.dot_general(
            chosen,
            tok_all[...],
            (((0,), (0,)), ((), ())),
            preferred_element_type=jnp.float32,
        ).astype(jnp.bfloat16)

    @pl.loop(0, chips - 1)
    def _(step):
        offset = offset_of(step, chips)
        send_rows[offset] = pick(offset)
        remote(
            send_rows.at[offset],
            recv_rows.at[offset],
            row_send.at[offset],
            row_recv.at[offset],
            to_chip(offset),
        ).start()
        remote(
            flag_send,
            flag_recv.at[offset],
            flag_ssem.at[offset],
            flag_rsem.at[offset],
            to_chip(offset),
        ).start()

    recv_rows[0] = pick(0)

    block = gate_mat.shape[0] // gate_scale.shape[1]

    def dequant_in_place(copy, mat, scale_at):
        copy.wait()

        @pl.loop(0, mat.shape[0] // block)
        def _(piece):
            at = pl.ds(pl.multiple_of(piece * block, block), block)
            for column in range(mat.shape[1] // block):
                lanes_at = slice(column * block, (column + 1) * block)
                mat[at, lanes_at] = (
                    mat[at, lanes_at].astype(jnp.float32) * scale_at(piece, column)
                ).astype(jnp.bfloat16)

    dequant_in_place(weight_copies[0], gate_mat, lambda row, column: gate_scale[column, row])
    dequant_in_place(weight_copies[1], up_mat, lambda row, column: up_scale[column, row])
    dequant_in_place(weight_copies[2], down_mat, lambda row, column: down_scale[row, column])

    def first_half(offset):
        features = recv_rows[offset]
        part_out[offset, :, 0:hidden_size] = jnp.dot(
            features, gate_mat[...], preferred_element_type=jnp.float32
        ).astype(jnp.bfloat16)
        part_out[offset, :, hidden_size:] = jnp.dot(
            features, up_mat[...], preferred_element_type=jnp.float32
        ).astype(jnp.bfloat16)
        part_copy(offset).start()

    def part_copy(offset):
        return remote(
            part_out.at[offset],
            part_in.at[offset],
            part_send.at[offset],
            part_recv.at[offset],
            partner,
        )

    def second_half(offset):
        part_copy(offset).wait()
        gate = part_out[offset, :, 0:hidden_size].astype(jnp.float32) + part_in[
            offset, :, 0:hidden_size
        ].astype(jnp.float32)
        up = part_out[offset, :, hidden_size:].astype(jnp.float32) + part_in[
            offset, :, hidden_size:
        ].astype(jnp.float32)
        hidden = (gate * (1.0 / (1.0 + jnp.exp(-gate))) * up).astype(jnp.bfloat16)
        return jnp.dot(hidden, down_mat[...], preferred_element_type=jnp.float32).astype(
            jnp.bfloat16
        )

    def row_copy(offset):
        return remote(
            send_rows.at[offset],
            recv_rows.at[offset],
            row_send.at[offset],
            row_recv.at[offset],
            to_chip(offset),
        )

    def back_copy(offset):
        return remote(
            hidden_out.at[offset],
            returned.at[offset],
            back_send.at[offset],
            back_recv.at[offset],
            from_chip(offset),
        )

    first_half(0)

    @pl.loop(0, chips - 1)
    def _(step):
        offset = offset_of(step, chips)
        row_copy(offset).wait()
        first_half(offset)
        before = jnp.where(step == 0, 0, offset_of(step - 1, chips))
        result = second_half(before)

        @pl.when(step == 0)
        def _():
            returned[0] = result

        @pl.when(step > 0)
        def _():
            hidden_out[before] = result
            back_copy(before).start()

    last = offset_of(chips - 2, chips)
    hidden_out[last] = second_half(last)
    back_copy(last).start()

    flag_recv[0] = flag_send[...]

    @pl.loop(1, chips)
    def _(offset):
        remote(
            flag_send,
            flag_recv.at[offset],
            flag_ssem.at[offset],
            flag_rsem.at[offset],
            to_chip(offset),
        ).wait()

    flag_far[0] = jnp.max(flag_recv[...], axis=0)
    far_copies = [
        remote(
            flag_far.at[0],
            flag_far.at[far],
            far_ssem.at[far],
            far_rsem.at[far],
            {"groups": lax.rem(group + far, groups)},
        )
        for far in range(1, groups)
    ]
    for copy in far_copies:
        copy.start()
    total[...] = jnp.zeros_like(total)

    def add_returned(offset):
        in_a, in_b = slot_columns(lax.rem(chip + offset, chips))
        weight = jnp.where(in_a, info_all[:, 2:3], 0.0) + jnp.where(
            in_b, info_all[:, 3:4], 0.0
        )
        high = weight.astype(jnp.bfloat16)
        low = (weight - high.astype(jnp.float32)).astype(jnp.bfloat16)
        values = returned[offset]
        total[...] += jnp.dot(high, values, preferred_element_type=jnp.float32) + jnp.dot(
            low, values, preferred_element_type=jnp.float32
        )

    add_returned(0)

    @pl.loop(0, chips - 1)
    def _(step):
        offset = offset_of(step, chips)
        back_copy(offset).wait()
        add_returned(offset)

    mixed[...] = total[...].astype(jnp.bfloat16)
    own_out = pltpu.make_async_copy(
        mixed.at[my_rows, :], out.at[:, my_cols], local_sem.at[2]
    )
    pair_out = remote(
        mixed.at[your_rows, :],
        out.at[:, my_cols],
        pair_send.at[2],
        pair_recv.at[2],
        partner,
    )
    own_out.start()
    pair_out.start()

    for copy in far_copies:
        copy.wait()
    flag_out[0] = jnp.max(flag_far[...]).astype(jnp.int32)
    own_out.wait()
    pair_out.wait()


FAR_CHUNKS = 2
COLUMN_PARTS = 2


def two_level_kernel(
    groups,
    slots,
    tokens,
    host,
    copied,
    gate_prob,
    hot,
    w_gate,
    w_up,
    w_down,
    gate_scale,
    up_scale,
    down_scale,
    out,
    flag_out,
    tok_all,
    far_tok,
    info_rows,
    pool_info,
    pool_rank,
    gate_mat,
    up_mat,
    down_mat,
    send_rows,
    recv_rows,
    part_out,
    part_in,
    hidden_out,
    returned,
    sum_out,
    sum_in,
    total,
    mixed,
    flag_send,
    flag_recv,
    flag_far,
    local_sem,
    weight_sem,
    pair_send,
    pair_recv,
    info_send,
    info_recv,
    far_send,
    far_recv,
    row_send,
    row_recv,
    part_send,
    part_recv,
    back_send,
    back_recv,
    sum_send,
    sum_recv,
    out_sem,
    out_send,
    out_recv,
    flag_ssem,
    flag_rsem,
    far_ssem,
    far_rsem,
):
    cores = SPLIT
    chips = lax.axis_size("ep") // cores
    rows = tokens.shape[0]
    half = tokens.shape[1] // cores
    piece = half // COLUMN_PARTS
    few = rows // FAR_CHUNKS
    pooled = cores * rows
    hidden_size = gate_mat.shape[1]
    top_count = host.shape[0]
    me = lax.axis_index("ep")
    group = lax.axis_index("groups")
    chip = me // cores
    core = me % cores
    other = 1 - core
    column = chip % 2
    level = chip // 2
    side = level // 2
    inner = (level == 1) | (level == 2)
    outer_index = jnp.where(inner, 0, 1)
    far_inner = (2 - side) * 2 + column
    far_outer = 3 * (1 - side) * 2 + column
    partner = {"ep": chip * cores + other}

    def at_chip(which, which_core=None):
        return {"ep": which * cores + (core if which_core is None else which_core)}

    def remote(source, target, send, recv, device):
        return pltpu.make_async_remote_copy(
            src_ref=source,
            dst_ref=target,
            send_sem=send,
            recv_sem=recv,
            device_id=device,
            device_id_type=pl.DeviceIdType.MESH,
        )

    weight_copies = [
        pltpu.make_async_copy(w_gate.at[0], gate_mat, weight_sem.at[0]),
        pltpu.make_async_copy(w_up.at[0], up_mat, weight_sem.at[1]),
        pltpu.make_async_copy(w_down.at[0], down_mat, weight_sem.at[2]),
    ]
    my_rows = pl.ds(pl.multiple_of(core * rows, rows), rows)
    my_cols = pl.ds(pl.multiple_of(core * half, 128), half)
    your_cols = pl.ds(pl.multiple_of(other * half, 128), half)
    own_tok = pltpu.make_async_copy(
        tokens.at[:, my_cols], tok_all.at[my_rows, :], local_sem.at[0]
    )

    barrier = pltpu.get_barrier_semaphore()
    devices = cores * chips
    for far in range(1, groups):
        pl.semaphore_signal(
            barrier,
            inc=1,
            device_id={"groups": lax.rem(group + far, groups)},
            device_id_type=pl.DeviceIdType.MESH,
        )

    @pl.loop(1, devices)
    def _(step):
        pl.semaphore_signal(
            barrier,
            inc=1,
            device_id={"ep": lax.rem(me + step, devices)},
            device_id_type=pl.DeviceIdType.MESH,
        )

    own_tok.start()
    for copy in weight_copies:
        copy.start()
    named = host[...]
    moved = jnp.zeros_like(named)
    for name in range(chips):
        moved = jnp.where(named == name, hot[name], moved)
    expert = jnp.where(copied[...] == 0, named, moved).astype(jnp.float32)
    info_rows[core] = jnp.concatenate(
        [expert, gate_prob[...], jnp.zeros((8 - 2 * top_count, rows), jnp.float32)], axis=0
    )
    pl.semaphore_wait(barrier, devices + groups - 2)

    def far_copy(chunk, part, target):
        return remote(
            tokens.at[
                pl.ds(pl.multiple_of(chunk * few, few), few),
                pl.ds(pl.multiple_of(target * half + part * piece, 128), piece),
            ],
            far_tok.at[
                chunk,
                pl.ds(pl.multiple_of((outer_index * cores + core) * few, few), few),
                pl.ds(pl.multiple_of(part * piece, 128), piece),
            ],
            far_send.at[(chunk * COLUMN_PARTS + part) * cores + target],
            far_recv.at[(chunk * COLUMN_PARTS + part) * 2 * cores + outer_index * cores + core],
            at_chip(far_inner, target),
        )

    def far_arrival(chunk, part, source):
        return remote(
            tokens.at[pl.ds(0, few), pl.ds(0, piece)],
            far_tok.at[
                chunk,
                pl.ds(pl.multiple_of(source * few, few), few),
                pl.ds(pl.multiple_of(part * piece, 128), piece),
            ],
            far_send.at[0],
            far_recv.at[(chunk * COLUMN_PARTS + part) * 2 * cores + source],
            partner,
        )

    def far_info(target):
        return remote(
            info_rows.at[core],
            info_rows.at[cores + outer_index * cores + core],
            info_send.at[target],
            info_recv.at[outer_index * cores + core],
            at_chip(far_inner, target),
        )

    pair_info = remote(
        info_rows.at[core], info_rows.at[core], pair_send.at[0], pair_recv.at[0], partner
    )
    pair_tok = remote(
        tokens.at[:, your_cols],
        tok_all.at[my_rows, :],
        pair_send.at[1],
        pair_recv.at[1],
        partner,
    )
    pair_info.start()
    for target in range(cores):
        far_info(target).start()
    pair_tok.start()

    @pl.loop(0, FAR_CHUNKS * COLUMN_PARTS)
    def _(step):
        for target in range(cores):
            far_copy(step // COLUMN_PARTS, step % COLUMN_PARTS, target).start()

    expert_ids = lax.broadcasted_iota(jnp.int32, (chips, pooled), 0)
    near = (expert_ids // 4 == side).astype(jnp.float32)
    before = (
        lax.broadcasted_iota(jnp.int32, (pooled, pooled), 0)
        < lax.broadcasted_iota(jnp.int32, (pooled, pooled), 1)
    ).astype(jnp.float32).astype(jnp.bfloat16)

    def rank_pool(pool, info):
        pool_info[pool] = info
        names = expert_ids.astype(jnp.float32)
        hot_a = (info[0:1, :] == names).astype(jnp.float32)
        hot_b = (info[1:2, :] == names).astype(jnp.float32)
        both = jnp.concatenate([hot_a, hot_b], axis=0).astype(jnp.bfloat16)
        ranks = jnp.dot(both, before, preferred_element_type=jnp.float32)
        count_a = jnp.sum(hot_a, axis=1, keepdims=True)
        count_b = jnp.sum(hot_b, axis=1, keepdims=True)
        pool_rank[pool, 0:chips, :] = hot_a * (ranks[0:chips] + 1.0)
        pool_rank[pool, chips:, :] = hot_b * (ranks[chips:] + count_a + 1.0)
        counts = (count_a + count_b) * near
        return jnp.max(jnp.max(counts, axis=1, keepdims=True), axis=0, keepdims=True)

    def flag_of(most):
        return jnp.broadcast_to((most > slots).astype(jnp.float32), flag_send.shape)

    positions = lax.broadcasted_iota(jnp.int32, (slots, pooled), 0).astype(jnp.float32) + 1.0

    def slot_rows(pool, mask):
        mine = expert_ids == (chip ^ mask)
        row_a = jnp.sum(
            jnp.where(mine, pool_rank[pool, 0:chips, :], 0.0), axis=0, keepdims=True
        )
        row_b = jnp.sum(jnp.where(mine, pool_rank[pool, chips:, :], 0.0), axis=0, keepdims=True)
        return row_a == positions, row_b == positions

    def chosen_rows(pool, mask):
        in_a, in_b = slot_rows(pool, mask)
        return (in_a | in_b).astype(jnp.float32).astype(jnp.bfloat16)

    def own_row_copy(mask):
        return remote(
            send_rows.at[mask],
            recv_rows.at[mask],
            row_send.at[mask * COLUMN_PARTS],
            row_recv.at[mask * COLUMN_PARTS],
            at_chip(chip ^ mask),
        )

    pair_info.wait()
    own_most = rank_pool(0, jnp.concatenate([info_rows[0], info_rows[1]], axis=1))
    flag_send[...] = flag_of(own_most)
    own_tok.wait()
    pair_tok.wait()

    def pick_own(mask):
        return jnp.dot(
            chosen_rows(0, mask), tok_all[...], preferred_element_type=jnp.float32
        ).astype(jnp.bfloat16)

    @pl.loop(0, 3)
    def _(step):
        mask = lax.rem(step + 1, 3) + 1
        send_rows[mask] = pick_own(mask)
        own_row_copy(mask).start()

    recv_rows[0] = pick_own(0)

    @pl.when(inner)
    def _():
        for source in range(2 * cores):
            remote(
                info_rows.at[0],
                info_rows.at[cores + source],
                info_send.at[0],
                info_recv.at[source],
                partner,
            ).wait_recv()
        left = lax.broadcasted_iota(jnp.int32, (8, rows), 1) < few
        turned = [pltpu.roll(info_rows[cores + source], few, 1) for source in range(2 * cores)]
        first = [
            jnp.where(left, info_rows[cores + 2 * pair], turned[2 * pair + 1])
            for pair in range(cores)
        ]
        second = [
            jnp.where(left, turned[2 * pair], info_rows[cores + 2 * pair + 1])
            for pair in range(cores)
        ]
        most_a = rank_pool(1, jnp.concatenate(first, axis=1))
        most_b = rank_pool(2, jnp.concatenate(second, axis=1))
        flag_send[...] = flag_of(jnp.maximum(own_most, jnp.maximum(most_a, most_b)))

    def flag_copy(offset):
        return remote(
            flag_send,
            flag_recv.at[offset],
            flag_ssem.at[offset],
            flag_rsem.at[offset],
            at_chip(lax.rem(chip + offset, chips)),
        )

    @pl.loop(1, chips)
    def _(offset):
        flag_copy(offset).start()

    block = gate_mat.shape[0] // gate_scale.shape[1]

    def dequant_in_place(copy, mat, scale_at):
        copy.wait()

        @pl.loop(0, mat.shape[0] // block)
        def _(strip):
            at = pl.ds(pl.multiple_of(strip * block, block), block)
            for lane_block in range(mat.shape[1] // block):
                lanes_at = slice(lane_block * block, (lane_block + 1) * block)
                mat[at, lanes_at] = (
                    mat[at, lanes_at].astype(jnp.float32) * scale_at(strip, lane_block)
                ).astype(jnp.bfloat16)

    dequant_in_place(weight_copies[0], gate_mat, lambda row, lane: gate_scale[lane, row])
    dequant_in_place(weight_copies[1], up_mat, lambda row, lane: up_scale[lane, row])
    dequant_in_place(weight_copies[2], down_mat, lambda row, lane: down_scale[row, lane])

    def part_cols(part):
        return pl.ds(pl.multiple_of(part * piece, 128), piece)

    def relay_copy(chunk, mask, part):
        target_group = 4 + 2 * chunk + mask % 2
        return remote(
            send_rows.at[4 + 4 * chunk + mask, :, part_cols(part)],
            recv_rows.at[target_group, :, part_cols(part)],
            row_send.at[(4 + 4 * chunk + mask) * COLUMN_PARTS + part],
            row_recv.at[target_group * COLUMN_PARTS + part],
            at_chip(chip ^ mask),
        )

    def relay(chunk):
        @pl.loop(0, COLUMN_PARTS)
        def _(part):
            for source in range(2 * cores):
                far_arrival(chunk, part, source).wait_recv()

            @pl.loop(0, 4)
            def _(step):
                mask = jnp.where(step < 2, step + 2, 3 - step)
                picked = jnp.dot(
                    chosen_rows(1 + chunk, mask),
                    far_tok[chunk, :, part_cols(part)],
                    preferred_element_type=jnp.float32,
                ).astype(jnp.bfloat16)

                @pl.when(mask == 0)
                def _():
                    recv_rows[4 + 2 * chunk, :, part_cols(part)] = picked

                @pl.when(mask != 0)
                def _():
                    send_rows[4 + 4 * chunk + mask, :, part_cols(part)] = picked
                    relay_copy(chunk, mask, part).start()

    def wait_rows(slot_group):
        @pl.when((slot_group > 0) & (slot_group < 4))
        def _():
            own_row_copy(slot_group).wait_recv()

        @pl.when((slot_group >= 4) & ~(inner & (slot_group % 2 == 0)))
        def _():
            for part in range(COLUMN_PARTS):
                remote(
                    send_rows.at[0, :, part_cols(part)],
                    recv_rows.at[slot_group, :, part_cols(part)],
                    row_send.at[0],
                    row_recv.at[slot_group * COLUMN_PARTS + part],
                    partner,
                ).wait_recv()

    def part_copy(slot_group):
        return remote(
            part_out.at[slot_group],
            part_in.at[slot_group],
            part_send.at[slot_group],
            part_recv.at[slot_group],
            partner,
        )

    def first_half(slot_group):
        wait_rows(slot_group)
        features = recv_rows[slot_group]
        part_out[slot_group, :, 0:hidden_size] = jnp.dot(
            features, gate_mat[...], preferred_element_type=jnp.float32
        ).astype(jnp.bfloat16)
        part_out[slot_group, :, hidden_size:] = jnp.dot(
            features, up_mat[...], preferred_element_type=jnp.float32
        ).astype(jnp.bfloat16)
        part_copy(slot_group).start()

    def home_of(slot_group):
        own = slot_group < 4
        mask = jnp.where(own, slot_group, slot_group % 2 + jnp.where(inner, 0, 2))
        pool = jnp.where(own, 0, slot_group // 2 - 1)
        return pool, mask

    def back_copy(slot_group, part):
        pool, mask = home_of(slot_group)
        return remote(
            hidden_out.at[slot_group, :, part_cols(part)],
            returned.at[pool * 4 + mask, :, part_cols(part)],
            back_send.at[slot_group * COLUMN_PARTS + part],
            back_recv.at[(pool * 4 + mask) * COLUMN_PARTS + part],
            at_chip(chip ^ mask),
        )

    def second_half(slot_group):
        part_copy(slot_group).wait()
        gate = part_out[slot_group, :, 0:hidden_size].astype(jnp.float32) + part_in[
            slot_group, :, 0:hidden_size
        ].astype(jnp.float32)
        up = part_out[slot_group, :, hidden_size:].astype(jnp.float32) + part_in[
            slot_group, :, hidden_size:
        ].astype(jnp.float32)
        hidden = (gate * (1.0 / (1.0 + jnp.exp(-gate))) * up).astype(jnp.bfloat16)
        pool, mask = home_of(slot_group)
        for part in range(COLUMN_PARTS):
            cols = slice(part * piece, (part + 1) * piece)
            result = jnp.dot(
                hidden, down_mat[:, cols], preferred_element_type=jnp.float32
            ).astype(jnp.bfloat16)

            @pl.when(mask == 0)
            def _():
                returned[pool * 4, :, cols] = result

            @pl.when(mask != 0)
            def _():
                hidden_out[slot_group, :, cols] = result
                back_copy(slot_group, part).start()

    def back_arrival(pool, mask, part):
        return remote(
            hidden_out.at[0, :, part_cols(part)],
            returned.at[pool * 4 + mask, :, part_cols(part)],
            back_send.at[0],
            back_recv.at[(pool * 4 + mask) * COLUMN_PARTS + part],
            partner,
        )

    def combined(pool, part):
        acc = None
        for mask in range(4):
            if mask:
                back_arrival(pool, mask, part).wait_recv()
            in_a, in_b = slot_rows(pool, mask)
            weight = jnp.where(in_a, pool_info[pool, top_count : top_count + 1, :], 0.0)
            weight += jnp.where(in_b, pool_info[pool, top_count + 1 : top_count + 2, :], 0.0)
            high = weight.astype(jnp.bfloat16)
            low = (weight - high.astype(jnp.float32)).astype(jnp.bfloat16)
            values = returned[pool * 4 + mask, :, part_cols(part)]
            for term in (high, low):
                product = lax.dot_general(
                    term, values, (((0,), (0,)), ((), ())), preferred_element_type=jnp.float32
                )
                acc = product if acc is None else acc + product
        return acc

    def sum_copy(chunk, part, which):
        return remote(
            sum_out.at[chunk, which * rows : (which + 1) * rows, part_cols(part)],
            sum_in.at[chunk, :, part_cols(part)],
            sum_send.at[(chunk * COLUMN_PARTS + part) * 2 + which],
            sum_recv.at[chunk * COLUMN_PARTS + part],
            at_chip(far_outer if which else far_inner),
        )

    def return_sums(chunk):
        @pl.loop(0, COLUMN_PARTS)
        def _(part):
            sum_out[chunk, :, part_cols(part)] = combined(1 + chunk, part).astype(jnp.bfloat16)
            for which in range(2):
                sum_copy(chunk, part, which).start()

    @pl.loop(0, 5)
    def _(turn):
        @pl.when(inner & (turn >= 1) & (turn <= FAR_CHUNKS))
        def _():
            relay(turn - 1)

        @pl.when(inner & (turn >= 3))
        def _():
            return_sums(turn - 3)

        @pl.when(turn < 4)
        def _():
            position = jnp.where(
                inner & (turn >= 1), jnp.where(turn == 3, 1, turn + 1), turn
            )

            @pl.loop(0, 2)
            def _(which):
                first_half(2 * position + which)

            @pl.loop(0, 2)
            def _(which):
                second_half(2 * position + which)

    flag_recv[0] = flag_send[...]

    @pl.loop(1, chips)
    def _(offset):
        flag_copy(offset).wait()

    flag_far[0] = jnp.max(flag_recv[...], axis=0)
    far_copies = [
        remote(
            flag_far.at[0],
            flag_far.at[far],
            far_ssem.at[far],
            far_rsem.at[far],
            {"groups": lax.rem(group + far, groups)},
        )
        for far in range(1, groups)
    ]
    for copy in far_copies:
        copy.start()

    @pl.loop(0, COLUMN_PARTS)
    def _(part):
        total[:, part_cols(part)] = combined(0, part)

    def out_rows(owner, chunk):
        return pl.ds(pl.multiple_of(owner * rows + chunk * few, few), few)

    def out_cols(part):
        return pl.ds(pl.multiple_of(core * half + part * piece, 128), piece)

    def own_out(chunk, part):
        return pltpu.make_async_copy(
            mixed.at[out_rows(core, chunk), part_cols(part)],
            out.at[chunk * few : (chunk + 1) * few, out_cols(part)],
            out_sem.at[chunk * COLUMN_PARTS + part],
        )

    def pair_out(chunk, part):
        return remote(
            mixed.at[out_rows(other, chunk), part_cols(part)],
            out.at[chunk * few : (chunk + 1) * few, out_cols(part)],
            out_send.at[chunk * COLUMN_PARTS + part],
            out_recv.at[chunk * COLUMN_PARTS + part],
            partner,
        )

    for chunk in range(FAR_CHUNKS):
        for part in range(COLUMN_PARTS):
            cols = slice(part * piece, (part + 1) * piece)
            remote(
                sum_out.at[0, 0:rows, cols],
                sum_in.at[chunk, :, cols],
                sum_send.at[0],
                sum_recv.at[chunk * COLUMN_PARTS + part],
                partner,
            ).wait_recv()
            for owner in range(cores):
                at = slice(owner * rows + chunk * few, owner * rows + (chunk + 1) * few)
                mixed[at, cols] = (
                    total[at, cols]
                    + sum_in[chunk, owner * few : (owner + 1) * few, cols].astype(jnp.float32)
                ).astype(jnp.bfloat16)
            pair_out(chunk, part).start()
            own_out(chunk, part).start()

    for copy in far_copies:
        copy.wait()
    flag_out[0] = jnp.max(flag_far[...]).astype(jnp.int32)

    for target in range(cores):
        far_info(target).wait_send()

    @pl.loop(0, FAR_CHUNKS * COLUMN_PARTS)
    def _(step):
        for target in range(cores):
            far_copy(step // COLUMN_PARTS, step % COLUMN_PARTS, target).wait_send()

    @pl.loop(1, 4)
    def _(mask):
        own_row_copy(mask).wait_send()

    @pl.loop(0, 8)
    def _(slot_group):
        _, mask = home_of(slot_group)

        @pl.when(mask != 0)
        def _():
            for part in range(COLUMN_PARTS):
                back_copy(slot_group, part).wait_send()

    @pl.when(inner)
    def _():
        @pl.loop(0, FAR_CHUNKS * COLUMN_PARTS)
        def _(step):
            chunk = step // COLUMN_PARTS
            part = step % COLUMN_PARTS
            for which in range(2):
                sum_copy(chunk, part, which).wait_send()

            @pl.loop(1, 4)
            def _(mask):
                relay_copy(chunk, mask, part).wait_send()

    for chunk in range(FAR_CHUNKS):
        for part in range(COLUMN_PARTS):
            own_out(chunk, part).wait()
            pair_out(chunk, part).wait()


def two_level_call(slots, tok_rows, half, hidden_size, groups, weight_shapes):
    cores = SPLIT
    chips = lax.axis_size("ep") // cores
    pooled = cores * tok_rows
    dma = pltpu.SemaphoreType.DMA
    pieces = FAR_CHUNKS * COLUMN_PARTS
    any_space = pl.BlockSpec(memory_space=pl.ANY)
    vmem_space = pl.BlockSpec(memory_space=pltpu.VMEM)
    smem_space = pl.BlockSpec(memory_space=pltpu.SMEM)
    bf16, f32 = jnp.bfloat16, jnp.float32
    return pl.pallas_call(
        functools.partial(two_level_kernel, groups, slots),
        out_shape=(
            jax.ShapeDtypeStruct((tok_rows, cores * half), bf16),
            jax.ShapeDtypeStruct((1,), jnp.int32),
        ),
        in_specs=[any_space] + [vmem_space] * 3 + [smem_space] + [any_space] * 3 + [smem_space] * 3,
        out_specs=(any_space, smem_space),
        scratch_shapes=[
            pltpu.VMEM((pooled, half), bf16),
            pltpu.VMEM((FAR_CHUNKS, pooled, half), bf16),
            pltpu.VMEM((3 * cores, 8, tok_rows), f32),
            pltpu.VMEM((3, 8, pooled), f32),
            pltpu.VMEM((3, 2 * chips, pooled), f32),
            pltpu.VMEM(weight_shapes[0], bf16),
            pltpu.VMEM(weight_shapes[1], bf16),
            pltpu.VMEM(weight_shapes[2], bf16),
            pltpu.VMEM((12, slots, half), bf16),
            pltpu.VMEM((8, slots, half), bf16),
            pltpu.VMEM((8, slots, 2 * hidden_size), bf16),
            pltpu.VMEM((8, slots, 2 * hidden_size), bf16),
            pltpu.VMEM((8, slots, half), bf16),
            pltpu.VMEM((12, slots, half), bf16),
            pltpu.VMEM((FAR_CHUNKS, pooled, half), bf16),
            pltpu.VMEM((FAR_CHUNKS, tok_rows, half), bf16),
            pltpu.VMEM((pooled, half), f32),
            pltpu.VMEM((pooled, half), bf16),
            pltpu.VMEM((8, 128), f32),
            pltpu.VMEM((chips, 8, 128), f32),
            pltpu.VMEM((groups, 8, 128), f32),
            dma((1,)),
            dma((3,)),
            dma((2,)),
            dma((2,)),
            dma((cores,)),
            dma((2 * cores,)),
            dma((pieces * cores,)),
            dma((pieces * 2 * cores,)),
            dma((12 * COLUMN_PARTS,)),
            dma((8 * COLUMN_PARTS,)),
            dma((8,)),
            dma((8,)),
            dma((8 * COLUMN_PARTS,)),
            dma((12 * COLUMN_PARTS,)),
            dma((pieces * 2,)),
            dma((pieces,)),
            dma((pieces,)),
            dma((pieces,)),
            dma((pieces,)),
            dma((chips,)),
            dma((chips,)),
            dma((groups,)),
            dma((groups,)),
        ],
        compiler_params=pltpu.CompilerParams(
            collective_id=0, has_side_effects=True, vmem_limit_bytes=62 * 1024 * 1024
        ),
    )


def direct_call(chips, slots, tok_rows, half, hidden_size, groups, weight_shapes):
    cores = SPLIT
    width = cores * half
    pooled = cores * tok_rows
    any_space = pl.BlockSpec(memory_space=pl.ANY)
    vmem_space = pl.BlockSpec(memory_space=pltpu.VMEM)
    smem_space = pl.BlockSpec(memory_space=pltpu.SMEM)
    dma = pltpu.SemaphoreType.DMA
    return pl.pallas_call(
        functools.partial(fused_kernel, chips, cores, groups, slots),
        out_shape=(
            jax.ShapeDtypeStruct((tok_rows, width), jnp.bfloat16),
            jax.ShapeDtypeStruct((1,), jnp.int32),
        ),
        in_specs=[any_space] + [vmem_space] * 3 + [smem_space] + [any_space] * 3 + [smem_space] * 3,
        out_specs=(any_space, smem_space),
        scratch_shapes=[
            pltpu.VMEM((pooled, half), jnp.bfloat16),
            pltpu.VMEM((cores, 8, tok_rows), jnp.float32),
            pltpu.VMEM((pooled, 8), jnp.float32),
            pltpu.VMEM(weight_shapes[0], jnp.bfloat16),
            pltpu.VMEM(weight_shapes[1], jnp.bfloat16),
            pltpu.VMEM(weight_shapes[2], jnp.bfloat16),
            pltpu.VMEM((pooled, 128), jnp.float32),
            pltpu.VMEM((pooled, 128), jnp.float32),
            pltpu.VMEM((chips, slots, half), jnp.bfloat16),
            pltpu.VMEM((chips, slots, half), jnp.bfloat16),
            pltpu.VMEM((chips, slots, 2 * hidden_size), jnp.bfloat16),
            pltpu.VMEM((chips, slots, 2 * hidden_size), jnp.bfloat16),
            pltpu.VMEM((chips, slots, half), jnp.bfloat16),
            pltpu.VMEM((chips, slots, half), jnp.bfloat16),
            pltpu.VMEM((pooled, half), jnp.float32),
            pltpu.VMEM((pooled, half), jnp.bfloat16),
            pltpu.VMEM((8, 128), jnp.float32),
            pltpu.VMEM((chips, 8, 128), jnp.float32),
            pltpu.VMEM((groups, 8, 128), jnp.float32),
            dma((3,)),
            dma((3,)),
            dma((3,)),
            dma((3,)),
            dma((chips,)),
            dma((chips,)),
            dma((chips,)),
            dma((chips,)),
            dma((chips,)),
            dma((chips,)),
            dma((chips,)),
            dma((chips,)),
            dma((groups,)),
            dma((groups,)),
        ],
        compiler_params=pltpu.CompilerParams(
            collective_id=0, has_side_effects=True, vmem_limit_bytes=60 * 1024 * 1024
        ),
    )


def two_level_fits(chips, tok_rows, half):
    return chips == 8 and tok_rows == 128 and half % (128 * COLUMN_PARTS) == 0


def per_device(
    tokens, host, copy, gate_prob, hot, w_gate, w_up, w_down, gate_scale, up_scale, down_scale
):
    cores = SPLIT
    chips = lax.axis_size("ep") // cores
    groups = lax.axis_size("groups")
    tok_rows, width = tokens.shape
    half = width // cores
    hidden_size = w_gate.shape[2]
    pooled = cores * tok_rows
    slots = pooled_slots(pooled, host.shape[1], chips)
    args = (
        tokens,
        host.T,
        copy.T,
        gate_prob.T,
        hot,
        w_gate,
        w_up,
        w_down,
        gate_scale[0].T,
        up_scale[0].T,
        down_scale[0],
    )
    weight_shapes = (w_gate.shape[1:], w_up.shape[1:], w_down.shape[1:])
    if two_level_fits(chips, tok_rows, half):
        call = two_level_call(slots, tok_rows, half, hidden_size, groups, weight_shapes)
    else:
        call = direct_call(chips, slots, tok_rows, half, hidden_size, groups, weight_shapes)
    out, flag = call(*args)
    return lax.cond(
        flag[0] > 0,
        lambda: padded_exchange(
            tokens,
            host,
            copy,
            gate_prob,
            hot,
            w_gate,
            w_up,
            w_down,
            gate_scale,
            up_scale,
            down_scale,
        ),
        lambda: out,
    )


def solution(mesh):
    return jax.shard_map(
        per_device,
        mesh=mesh,
        in_specs=(
            P(("groups", "ep"), None),
            P(("groups", "ep"), None),
            P(("groups", "ep"), None),
            P(("groups", "ep"), None),
            P(),
            P("ep", None, None),
            P("ep", None, None),
            P("ep", None, None),
            P("ep", None, None),
            P("ep", None, None),
            P("ep", None, None),
        ),
        out_specs=P(("groups", "ep"), None),
        check_vma=False,
    )
```

```python
import functools

import jax
import jax.numpy as jnp
from jax import lax
from jax.experimental import pallas as pl
from jax.experimental.pallas import tpu as pltpu
from jax.sharding import PartitionSpec as P

SPLIT = 2


def from_partner(value, axis, apart):
    mask = 2**apart
    pairs = [(source, source ^ mask) for source in range(lax.axis_size(axis))]
    return lax.ppermute(value, axis, pairs)


def dequant(weight, scales):
    rows_in, cols_in = weight.shape
    row_blocks, col_blocks = scales.shape
    expanded = jnp.repeat(scales, cols_in // col_blocks, axis=1)
    blocks = (
        weight.reshape(row_blocks, rows_in // row_blocks, cols_in).astype(jnp.float32)
        * expanded[:, None, :]
    )
    return blocks.reshape(rows_in, cols_in).astype(jnp.bfloat16)


def lookup(table_in, keys):
    positions = jnp.arange(table_in.shape[0], dtype=jnp.int32)
    return jnp.sum(jnp.where(keys[:, None] == positions[None, :], table_in[None, :], 0), axis=1)


def padded_exchange(
    tokens, host, copy, gate_prob, hot, w_gate, w_up, w_down, gate_scale, up_scale, down_scale
):
    devices = lax.axis_size("ep")
    experts = devices // SPLIT
    tok_rows, width = tokens.shape
    top_count = host.shape[1]
    capacity = tok_rows * top_count * 5 // (4 * experts)
    half_width = width // SPLIT
    pair_count = tok_rows * top_count
    host_f = host.reshape(pair_count)
    copy_f = copy.reshape(pair_count)
    onehot = (host_f[:, None] == jnp.arange(experts, dtype=jnp.int32)[None, :]).astype(jnp.int32)
    slot_f = jnp.sum((jnp.cumsum(onehot, axis=0) - 1) * onehot, axis=1)
    expert_f = jnp.where(copy_f == 0, host_f, lookup(hot, host_f))
    place_f = copy_f * capacity + slot_f
    tok_split = tokens.reshape(tok_rows, SPLIT, half_width)
    own_gate = dequant(w_gate[0], gate_scale[0])
    own_up = dequant(w_up[0], up_scale[0])
    own_down = dequant(w_down[0], down_scale[0])
    zone_rows = 2 * capacity
    slots_all = experts * zone_rows
    slot_table = (
        jnp.zeros((slots_all,), jnp.int32)
        .at[expert_f * zone_rows + place_f]
        .set(jnp.arange(pair_count, dtype=jnp.int32) + 1)
    )
    slot_table = slot_table.reshape(experts, zone_rows)
    filled = slot_table > 0
    row_of = jnp.maximum(slot_table - 1, 0) // top_count
    picked = tok_split[row_of[:, None, :], jnp.arange(SPLIT, dtype=jnp.int32)[None, :, None]]
    picked = jnp.where(filled[:, None, :, None], picked, jnp.zeros_like(picked))
    outgoing_rows = picked.reshape(devices, zone_rows, half_width)
    received = lax.all_to_all(outgoing_rows, "ep", split_axis=0, concat_axis=0, tiled=True)

    def project(matrix_in, own_mat):
        return jnp.dot(matrix_in, own_mat, preferred_element_type=jnp.float32)

    gate_part = project(received, own_gate).astype(jnp.bfloat16)
    up_part = project(received, own_up).astype(jnp.bfloat16)
    partner_gate, partner_up = from_partner((gate_part, up_part), "ep", 0)
    gate_sum = gate_part.astype(jnp.float32) + partner_gate.astype(jnp.float32)
    up_sum = up_part.astype(jnp.float32) + partner_up.astype(jnp.float32)
    hidden = (jax.nn.silu(gate_sum) * up_sum).astype(jnp.bfloat16)
    results = project(hidden, own_down).astype(jnp.bfloat16)
    returned = lax.all_to_all(results, "ep", split_axis=0, concat_axis=0, tiled=True)
    back_four = returned.reshape(experts, SPLIT, zone_rows, half_width)
    values = back_four[
        expert_f[:, None], jnp.arange(SPLIT, dtype=jnp.int32)[None, :], place_f[:, None]
    ]
    values = values.reshape(tok_rows, top_count, width).astype(jnp.float32)
    mixed = jnp.sum(values * gate_prob[:, :, None], axis=1)
    return mixed.astype(jnp.bfloat16)


def pooled_slots(chip_tokens, top_count, chips):
    mean = chip_tokens * top_count // chips
    return -(-(mean * 13 // 8) // 8) * 8


def offset_of(step, chips):
    return chips // 2 + ((step + 1) // 2) * (1 - 2 * (step % 2))


def fused_kernel(
    chips,
    cores,
    groups,
    slots,
    tokens,
    host,
    copied,
    gate_prob,
    hot,
    w_gate,
    w_up,
    w_down,
    gate_scale,
    up_scale,
    down_scale,
    out,
    flag_out,
    tok_all,
    info_rows,
    info_all,
    gate_mat,
    up_mat,
    down_mat,
    first_rank,
    second_rank,
    send_rows,
    recv_rows,
    part_out,
    part_in,
    hidden_out,
    returned,
    total,
    mixed,
    flag_send,
    flag_recv,
    flag_far,
    local_sem,
    weight_sem,
    pair_send,
    pair_recv,
    row_send,
    row_recv,
    part_send,
    part_recv,
    back_send,
    back_recv,
    flag_ssem,
    flag_rsem,
    far_ssem,
    far_rsem,
):
    rows = tokens.shape[0]
    half = tokens.shape[1] // cores
    hidden_size = gate_mat.shape[1]
    me = lax.axis_index("ep")
    group = lax.axis_index("groups")
    chip = me // cores
    core = me % cores
    other = 1 - core
    partner = {"ep": chip * cores + other}

    def to_chip(offset):
        return {"ep": lax.rem(chip + offset, chips) * cores + core}

    def from_chip(offset):
        return {"ep": lax.rem(chip + chips - offset, chips) * cores + core}

    weight_copies = [
        pltpu.make_async_copy(w_gate.at[0], gate_mat, weight_sem.at[0]),
        pltpu.make_async_copy(w_up.at[0], up_mat, weight_sem.at[1]),
        pltpu.make_async_copy(w_down.at[0], down_mat, weight_sem.at[2]),
    ]
    for copy in weight_copies:
        copy.start()
    my_rows = pl.ds(pl.multiple_of(core * rows, rows), rows)
    your_rows = pl.ds(pl.multiple_of(other * rows, rows), rows)
    my_cols = pl.ds(pl.multiple_of(core * half, 128), half)
    your_cols = pl.ds(pl.multiple_of(other * half, 128), half)
    own_tok = pltpu.make_async_copy(
        tokens.at[:, my_cols], tok_all.at[my_rows, :], local_sem.at[0]
    )
    own_tok.start()
    named = host[...]
    moved = jnp.zeros_like(named)
    for name in range(chips):
        moved = jnp.where(named == name, hot[name], moved)
    expert = jnp.where(copied[...] == 0, named, moved).astype(jnp.float32)
    top_count = named.shape[0]
    info_rows[core] = jnp.concatenate(
        [expert, gate_prob[...], jnp.zeros((8 - 2 * top_count, rows), jnp.float32)], axis=0
    )

    barrier = pltpu.get_barrier_semaphore()
    pl.semaphore_signal(
        barrier, inc=1, device_id=partner, device_id_type=pl.DeviceIdType.MESH
    )
    for far in range(1, groups):
        pl.semaphore_signal(
            barrier,
            inc=1,
            device_id={"groups": lax.rem(group + far, groups)},
            device_id_type=pl.DeviceIdType.MESH,
        )

    @pl.loop(1, chips)
    def _(offset):
        pl.semaphore_signal(
            barrier,
            inc=1,
            device_id=to_chip(offset),
            device_id_type=pl.DeviceIdType.MESH,
        )

    pl.semaphore_wait(barrier, chips + groups - 1)

    def remote(source, target, send, recv, device):
        return pltpu.make_async_remote_copy(
            src_ref=source,
            dst_ref=target,
            send_sem=send,
            recv_sem=recv,
            device_id=device,
            device_id_type=pl.DeviceIdType.MESH,
        )

    pair_info = remote(
        info_rows.at[core], info_rows.at[core], pair_send.at[0], pair_recv.at[0], partner
    )
    pair_tok = remote(
        tokens.at[:, your_cols],
        tok_all.at[my_rows, :],
        pair_send.at[1],
        pair_recv.at[1],
        partner,
    )
    pair_info.start()
    pair_tok.start()
    pair_info.wait()
    for part in range(cores):
        info_all[part * rows : (part + 1) * rows, :] = info_rows[part].T

    pooled = cores * rows
    lanes = lax.broadcasted_iota(jnp.int32, (pooled, 128), 1)
    expert_a = info_all[:, 0:1].astype(jnp.int32)
    expert_b = info_all[:, 1:2].astype(jnp.int32)
    match_a = expert_a == lanes
    match_b = expert_b == lanes
    hot_a = match_a.astype(jnp.float32)
    hot_b = match_b.astype(jnp.float32)
    below = (
        lax.broadcasted_iota(jnp.int32, (pooled, pooled), 1)
        < lax.broadcasted_iota(jnp.int32, (pooled, pooled), 0)
    ).astype(jnp.float32).astype(jnp.bfloat16)
    rank_a = jnp.dot(below, hot_a.astype(jnp.bfloat16), preferred_element_type=jnp.float32)
    rank_b = jnp.dot(below, hot_b.astype(jnp.bfloat16), preferred_element_type=jnp.float32)
    count_a = jnp.sum(hot_a, axis=0, keepdims=True)
    count_b = jnp.sum(hot_b, axis=0, keepdims=True)
    first_rank[...] = jnp.where(match_a, rank_a, -1.0)
    second_rank[...] = jnp.where(match_b, rank_b + count_a, -1.0)
    most = jnp.max(count_a + count_b, axis=1, keepdims=True)
    flag_send[...] = jnp.broadcast_to((most > slots).astype(jnp.float32), flag_send.shape)

    def slot_columns(expert):
        mine = lanes == expert
        column_a = jnp.sum(jnp.where(mine, first_rank[...] + 1.0, 0.0), axis=1, keepdims=True)
        column_b = jnp.sum(jnp.where(mine, second_rank[...] + 1.0, 0.0), axis=1, keepdims=True)
        positions = lax.broadcasted_iota(jnp.int32, (pooled, slots), 1).astype(jnp.float32) + 1.0
        return column_a == positions, column_b == positions

    own_tok.wait()
    pair_tok.wait()

    def pick(offset):
        in_a, in_b = slot_columns(lax.rem(chip + offset, chips))
        chosen = (in_a | in_b).astype(jnp.float32).astype(jnp.bfloat16)
        return lax.dot_general(
            chosen,
            tok_all[...],
            (((0,), (0,)), ((), ())),
            preferred_element_type=jnp.float32,
        ).astype(jnp.bfloat16)

    @pl.loop(0, chips - 1)
    def _(step):
        offset = offset_of(step, chips)
        send_rows[offset] = pick(offset)
        remote(
            send_rows.at[offset],
            recv_rows.at[offset],
            row_send.at[offset],
            row_recv.at[offset],
            to_chip(offset),
        ).start()
        remote(
            flag_send,
            flag_recv.at[offset],
            flag_ssem.at[offset],
            flag_rsem.at[offset],
            to_chip(offset),
        ).start()

    recv_rows[0] = pick(0)

    block = gate_mat.shape[0] // gate_scale.shape[1]

    def dequant_in_place(copy, mat, scale_at):
        copy.wait()

        @pl.loop(0, mat.shape[0] // block)
        def _(piece):
            at = pl.ds(pl.multiple_of(piece * block, block), block)
            for column in range(mat.shape[1] // block):
                lanes_at = slice(column * block, (column + 1) * block)
                mat[at, lanes_at] = (
                    mat[at, lanes_at].astype(jnp.float32) * scale_at(piece, column)
                ).astype(jnp.bfloat16)

    dequant_in_place(weight_copies[0], gate_mat, lambda row, column: gate_scale[column, row])
    dequant_in_place(weight_copies[1], up_mat, lambda row, column: up_scale[column, row])
    dequant_in_place(weight_copies[2], down_mat, lambda row, column: down_scale[row, column])

    def first_half(offset):
        features = recv_rows[offset]
        part_out[offset, :, 0:hidden_size] = jnp.dot(
            features, gate_mat[...], preferred_element_type=jnp.float32
        ).astype(jnp.bfloat16)
        part_out[offset, :, hidden_size:] = jnp.dot(
            features, up_mat[...], preferred_element_type=jnp.float32
        ).astype(jnp.bfloat16)
        part_copy(offset).start()

    def part_copy(offset):
        return remote(
            part_out.at[offset],
            part_in.at[offset],
            part_send.at[offset],
            part_recv.at[offset],
            partner,
        )

    def second_half(offset):
        part_copy(offset).wait()
        gate = part_out[offset, :, 0:hidden_size].astype(jnp.float32) + part_in[
            offset, :, 0:hidden_size
        ].astype(jnp.float32)
        up = part_out[offset, :, hidden_size:].astype(jnp.float32) + part_in[
            offset, :, hidden_size:
        ].astype(jnp.float32)
        hidden = (gate * (1.0 / (1.0 + jnp.exp(-gate))) * up).astype(jnp.bfloat16)
        return jnp.dot(hidden, down_mat[...], preferred_element_type=jnp.float32).astype(
            jnp.bfloat16
        )

    def row_copy(offset):
        return remote(
            send_rows.at[offset],
            recv_rows.at[offset],
            row_send.at[offset],
            row_recv.at[offset],
            to_chip(offset),
        )

    def back_copy(offset):
        return remote(
            hidden_out.at[offset],
            returned.at[offset],
            back_send.at[offset],
            back_recv.at[offset],
            from_chip(offset),
        )

    first_half(0)

    @pl.loop(0, chips - 1)
    def _(step):
        offset = offset_of(step, chips)
        row_copy(offset).wait()
        first_half(offset)
        before = jnp.where(step == 0, 0, offset_of(step - 1, chips))
        result = second_half(before)

        @pl.when(step == 0)
        def _():
            returned[0] = result

        @pl.when(step > 0)
        def _():
            hidden_out[before] = result
            back_copy(before).start()

    last = offset_of(chips - 2, chips)
    hidden_out[last] = second_half(last)
    back_copy(last).start()

    flag_recv[0] = flag_send[...]

    @pl.loop(1, chips)
    def _(offset):
        remote(
            flag_send,
            flag_recv.at[offset],
            flag_ssem.at[offset],
            flag_rsem.at[offset],
            to_chip(offset),
        ).wait()

    flag_far[0] = jnp.max(flag_recv[...], axis=0)
    far_copies = [
        remote(
            flag_far.at[0],
            flag_far.at[far],
            far_ssem.at[far],
            far_rsem.at[far],
            {"groups": lax.rem(group + far, groups)},
        )
        for far in range(1, groups)
    ]
    for copy in far_copies:
        copy.start()
    total[...] = jnp.zeros_like(total)

    def add_returned(offset):
        in_a, in_b = slot_columns(lax.rem(chip + offset, chips))
        weight = jnp.where(in_a, info_all[:, 2:3], 0.0) + jnp.where(
            in_b, info_all[:, 3:4], 0.0
        )
        high = weight.astype(jnp.bfloat16)
        low = (weight - high.astype(jnp.float32)).astype(jnp.bfloat16)
        values = returned[offset]
        total[...] += jnp.dot(high, values, preferred_element_type=jnp.float32) + jnp.dot(
            low, values, preferred_element_type=jnp.float32
        )

    add_returned(0)

    @pl.loop(0, chips - 1)
    def _(step):
        offset = offset_of(step, chips)
        back_copy(offset).wait()
        add_returned(offset)

    mixed[...] = total[...].astype(jnp.bfloat16)
    own_out = pltpu.make_async_copy(
        mixed.at[my_rows, :], out.at[:, my_cols], local_sem.at[2]
    )
    pair_out = remote(
        mixed.at[your_rows, :],
        out.at[:, my_cols],
        pair_send.at[2],
        pair_recv.at[2],
        partner,
    )
    own_out.start()
    pair_out.start()

    for copy in far_copies:
        copy.wait()
    flag_out[0] = jnp.max(flag_far[...]).astype(jnp.int32)
    own_out.wait()
    pair_out.wait()


FAR_CHUNKS = 2
INNER_TURNS = ((0,), (4, 1), (5,), (6, 2), (7,), (3,), (), ())
OUTER_TURNS = ((0, 1), (2,), (4, 5), (3,), (6, 7), (), (), ())
COLUMN_PARTS = 2


def two_level_kernel(
    groups,
    slots,
    tokens,
    host,
    copied,
    gate_prob,
    hot,
    w_gate,
    w_up,
    w_down,
    gate_scale,
    up_scale,
    down_scale,
    out,
    flag_out,
    tok_all,
    far_tok,
    info_rows,
    pool_info,
    pool_rank,
    gate_mat,
    up_mat,
    down_mat,
    send_rows,
    recv_rows,
    part_out,
    part_in,
    hidden_out,
    returned,
    sum_out,
    sum_in,
    total,
    mixed,
    flag_send,
    flag_recv,
    flag_far,
    local_sem,
    weight_sem,
    pair_send,
    pair_recv,
    info_send,
    info_recv,
    far_send,
    far_recv,
    row_send,
    row_recv,
    part_send,
    part_recv,
    back_send,
    back_recv,
    sum_send,
    sum_recv,
    out_sem,
    out_send,
    out_recv,
    flag_ssem,
    flag_rsem,
    far_ssem,
    far_rsem,
):
    cores = SPLIT
    chips = lax.axis_size("ep") // cores
    rows = tokens.shape[0]
    half = tokens.shape[1] // cores
    piece = half // COLUMN_PARTS
    pooled = cores * rows
    hidden_size = gate_mat.shape[1]
    top_count = host.shape[0]
    me = lax.axis_index("ep")
    group = lax.axis_index("groups")
    chip = me // cores
    core = me % cores
    other = 1 - core
    column = chip % 2
    level = chip // 2
    side = level // 2
    inner = (level == 1) | (level == 2)
    my_chunk = jnp.where(inner, 1, 0)
    far_inner = (2 - side) * 2 + column
    far_outer = 3 * (1 - side) * 2 + column
    partner = {"ep": chip * cores + other}

    def at_chip(which, which_core=None):
        return {"ep": which * cores + (core if which_core is None else which_core)}

    def remote(source, target, send, recv, device):
        return pltpu.make_async_remote_copy(
            src_ref=source,
            dst_ref=target,
            send_sem=send,
            recv_sem=recv,
            device_id=device,
            device_id_type=pl.DeviceIdType.MESH,
        )

    def part_cols(part):
        return pl.ds(pl.multiple_of(part * piece, 128), piece)

    weight_copies = [
        pltpu.make_async_copy(w_gate.at[0], gate_mat, weight_sem.at[0]),
        pltpu.make_async_copy(w_up.at[0], up_mat, weight_sem.at[1]),
        pltpu.make_async_copy(w_down.at[0], down_mat, weight_sem.at[2]),
    ]
    my_rows = pl.ds(pl.multiple_of(core * rows, rows), rows)
    my_cols = pl.ds(pl.multiple_of(core * half, 128), half)
    your_rows = pl.ds(pl.multiple_of(other * rows, rows), rows)
    your_cols = pl.ds(pl.multiple_of(other * half, 128), half)
    own_tok = pltpu.make_async_copy(
        tokens.at[:, my_cols], tok_all.at[my_rows, :], local_sem.at[0]
    )

    barrier = pltpu.get_barrier_semaphore()
    devices = cores * chips
    for far in range(1, groups):
        pl.semaphore_signal(
            barrier,
            inc=1,
            device_id={"groups": lax.rem(group + far, groups)},
            device_id_type=pl.DeviceIdType.MESH,
        )

    @pl.loop(1, devices)
    def _(step):
        pl.semaphore_signal(
            barrier,
            inc=1,
            device_id={"ep": lax.rem(me + step, devices)},
            device_id_type=pl.DeviceIdType.MESH,
        )

    own_tok.start()
    for copy in weight_copies:
        copy.start()
    named = host[...]
    moved = jnp.zeros_like(named)
    for name in range(chips):
        moved = jnp.where(named == name, hot[name], moved)
    expert = jnp.where(copied[...] == 0, named, moved).astype(jnp.float32)
    info_rows[core] = jnp.concatenate(
        [expert, gate_prob[...], jnp.zeros((8 - 2 * top_count, rows), jnp.float32)], axis=0
    )
    with jax.named_scope("k_barrier"):
        pl.semaphore_wait(barrier, devices + groups - 2)

    def far_copy(part, target):
        return remote(
            tokens.at[:, pl.ds(pl.multiple_of(target * half + part * piece, 128), piece)],
            far_tok.at[my_chunk, my_rows, part_cols(part)],
            far_send.at[part * cores + target],
            far_recv.at[(my_chunk * COLUMN_PARTS + part) * cores + core],
            at_chip(far_inner, target),
        )

    def far_arrival(chunk, part, source):
        return remote(
            tokens.at[:, pl.ds(0, piece)],
            far_tok.at[chunk, pl.ds(source * rows, rows), part_cols(part)],
            far_send.at[0],
            far_recv.at[(chunk * COLUMN_PARTS + part) * cores + source],
            partner,
        )

    def far_info(target):
        return remote(
            info_rows.at[core],
            info_rows.at[cores + my_chunk * cores + core],
            info_send.at[target],
            info_recv.at[my_chunk * cores + core],
            at_chip(far_inner, target),
        )

    def info_arrival(chunk, source):
        return remote(
            info_rows.at[0],
            info_rows.at[cores + chunk * cores + source],
            info_send.at[0],
            info_recv.at[chunk * cores + source],
            partner,
        )

    pair_info = remote(
        info_rows.at[core], info_rows.at[core], pair_send.at[0], pair_recv.at[0], partner
    )
    pair_tok = remote(
        tokens.at[:, your_cols],
        tok_all.at[my_rows, :],
        pair_send.at[1],
        pair_recv.at[1],
        partner,
    )
    pair_info.start()
    for target in range(cores):
        far_info(target).start()
    pair_tok.start()

    for part in range(COLUMN_PARTS):
        for target in range(cores):
            far_copy(part, target).start()

    expert_ids = lax.broadcasted_iota(jnp.int32, (chips, pooled), 0)
    near = (expert_ids // 4 == side).astype(jnp.float32)
    before = (
        lax.broadcasted_iota(jnp.int32, (pooled, pooled), 0)
        < lax.broadcasted_iota(jnp.int32, (pooled, pooled), 1)
    ).astype(jnp.float32).astype(jnp.bfloat16)

    flag_send[...] = jnp.zeros_like(flag_send)

    def rank_pool(pool):
        info = jnp.concatenate([info_rows[cores * pool + core] for core in range(cores)], axis=1)
        pool_info[pool] = info
        names = expert_ids.astype(jnp.float32)
        hot_a = (info[0:1, :] == names).astype(jnp.float32)
        hot_b = (info[1:2, :] == names).astype(jnp.float32)
        both = jnp.concatenate([hot_a, hot_b], axis=0).astype(jnp.bfloat16)
        ranks = jnp.dot(both, before, preferred_element_type=jnp.float32)
        count_a = jnp.sum(hot_a, axis=1, keepdims=True)
        count_b = jnp.sum(hot_b, axis=1, keepdims=True)
        pool_rank[pool, 0:chips, :] = hot_a * (ranks[0:chips] + 1.0)
        pool_rank[pool, chips:, :] = hot_b * (ranks[chips:] + count_a + 1.0)
        most = jnp.max((count_a + count_b) * near, axis=0, keepdims=True)[:, 0:128]
        flag_send[...] = jnp.maximum(flag_send[...], (most > slots).astype(jnp.float32))

    positions = lax.broadcasted_iota(jnp.int32, (slots, pooled), 0).astype(jnp.float32) + 1.0

    def slot_rows(pool, mask):
        mine = expert_ids == (chip ^ mask)
        row_a = jnp.sum(
            jnp.where(mine, pool_rank[pool, 0:chips, :], 0.0), axis=0, keepdims=True
        )
        row_b = jnp.sum(jnp.where(mine, pool_rank[pool, chips:, :], 0.0), axis=0, keepdims=True)
        return row_a == positions, row_b == positions

    def chosen_rows(pool, mask):
        in_a, in_b = slot_rows(pool, mask)
        return (in_a | in_b).astype(jnp.float32).astype(jnp.bfloat16)

    def own_row_copy(mask):
        return remote(
            send_rows.at[mask],
            recv_rows.at[mask],
            row_send.at[mask * COLUMN_PARTS],
            row_recv.at[mask * COLUMN_PARTS],
            at_chip(chip ^ mask),
        )

    with jax.named_scope("k_own_wait"):
        pair_info.wait()
        rank_pool(0)
        own_tok.wait()
        pair_tok.wait()

    def pick_own(mask):
        return jnp.dot(
            chosen_rows(0, mask), tok_all[...], preferred_element_type=jnp.float32
        ).astype(jnp.bfloat16)

    def send_own(mask):
        with jax.named_scope("k_own_pick"):
            send_rows[mask] = pick_own(mask)
            own_row_copy(mask).start()

    @pl.loop(0, jnp.where(inner, 2, 3))
    def _(step):
        send_own(jnp.where(step == 2, 3, 2 - step))

    recv_rows[0] = pick_own(0)

    def flag_copy(offset):
        return remote(
            flag_send,
            flag_recv.at[offset],
            flag_ssem.at[offset],
            flag_rsem.at[offset],
            at_chip(lax.rem(chip + offset, chips)),
        )

    block = gate_mat.shape[0] // gate_scale.shape[1]

    def dequant_in_place(copy, mat, scale_at):
        copy.wait()

        @pl.loop(0, mat.shape[0] // block)
        def _(strip):
            at = pl.ds(pl.multiple_of(strip * block, block), block)
            for lane_block in range(mat.shape[1] // block):
                lanes_at = slice(lane_block * block, (lane_block + 1) * block)
                mat[at, lanes_at] = (
                    mat[at, lanes_at].astype(jnp.float32) * scale_at(strip, lane_block)
                ).astype(jnp.bfloat16)

    with jax.named_scope("k_dequant"):
        dequant_in_place(weight_copies[0], gate_mat, lambda row, lane: gate_scale[lane, row])
        dequant_in_place(weight_copies[1], up_mat, lambda row, lane: up_scale[lane, row])
        dequant_in_place(weight_copies[2], down_mat, lambda row, lane: down_scale[row, lane])

    def relay_copy(chunk, mask, part):
        target_group = 4 + 2 * chunk + mask % 2
        return remote(
            send_rows.at[4 + 4 * chunk + mask, :, part_cols(part)],
            recv_rows.at[target_group, :, part_cols(part)],
            row_send.at[(4 + 4 * chunk + mask) * COLUMN_PARTS + part],
            row_recv.at[target_group * COLUMN_PARTS + part],
            at_chip(chip ^ mask),
        )

    def relay(chunk):
        with jax.named_scope("k_info_wait"):
            for source in range(cores):
                info_arrival(chunk, source).wait_recv()
        rank_pool(1 + chunk)

        @pl.loop(0, COLUMN_PARTS)
        def _(part):
            with jax.named_scope("k_far_wait"):
                for source in range(cores):
                    far_arrival(chunk, part, source).wait_recv()

            @pl.loop(0, 4)
            def _(step):
                mask = jnp.where(step < 2, step + 2, 3 - step)
                picked = jnp.dot(
                    chosen_rows(1 + chunk, mask),
                    far_tok[chunk, :, part_cols(part)],
                    preferred_element_type=jnp.float32,
                ).astype(jnp.bfloat16)

                @pl.when(mask == 0)
                def _():
                    recv_rows[4 + 2 * chunk, :, part_cols(part)] = picked

                @pl.when(mask != 0)
                def _():
                    send_rows[4 + 4 * chunk + mask, :, part_cols(part)] = picked
                    relay_copy(chunk, mask, part).start()

    def wait_rows(slot_group):
        @pl.when((slot_group > 0) & (slot_group < 4))
        def _():
            own_row_copy(slot_group).wait_recv()

        @pl.when((slot_group >= 4) & ~(inner & (slot_group % 2 == 0)))
        def _():
            for part in range(COLUMN_PARTS):
                remote(
                    send_rows.at[0, :, part_cols(part)],
                    recv_rows.at[slot_group, :, part_cols(part)],
                    row_send.at[0],
                    row_recv.at[slot_group * COLUMN_PARTS + part],
                    partner,
                ).wait_recv()

    def part_copy(slot_group):
        return remote(
            part_out.at[slot_group],
            part_in.at[slot_group],
            part_send.at[slot_group],
            part_recv.at[slot_group],
            partner,
        )

    def first_half(slot_group):
        with jax.named_scope("k_rows_wait"):
            wait_rows(slot_group)
        features = recv_rows[slot_group]
        part_out[slot_group, :, 0:hidden_size] = jnp.dot(
            features, gate_mat[...], preferred_element_type=jnp.float32
        ).astype(jnp.bfloat16)
        part_out[slot_group, :, hidden_size:] = jnp.dot(
            features, up_mat[...], preferred_element_type=jnp.float32
        ).astype(jnp.bfloat16)
        part_copy(slot_group).start()

    def home_of(slot_group):
        own = slot_group < 4
        mask = jnp.where(own, slot_group, slot_group % 2 + jnp.where(inner, 0, 2))
        pool = jnp.where(own, 0, slot_group // 2 - 1)
        return pool, mask

    def back_copy(slot_group, part):
        pool, mask = home_of(slot_group)
        return remote(
            hidden_out.at[slot_group, :, part_cols(part)],
            returned.at[pool * 4 + mask, :, part_cols(part)],
            back_send.at[slot_group * COLUMN_PARTS + part],
            back_recv.at[(pool * 4 + mask) * COLUMN_PARTS + part],
            at_chip(chip ^ mask),
        )

    def second_half(slot_group):
        with jax.named_scope("k_part_wait"):
            part_copy(slot_group).wait()
        gate = part_out[slot_group, :, 0:hidden_size].astype(jnp.float32) + part_in[
            slot_group, :, 0:hidden_size
        ].astype(jnp.float32)
        up = part_out[slot_group, :, hidden_size:].astype(jnp.float32) + part_in[
            slot_group, :, hidden_size:
        ].astype(jnp.float32)
        hidden = (gate * (1.0 / (1.0 + jnp.exp(-gate))) * up).astype(jnp.bfloat16)
        pool, mask = home_of(slot_group)
        for part in range(COLUMN_PARTS):
            cols = slice(part * piece, (part + 1) * piece)
            result = jnp.dot(
                hidden, down_mat[:, cols], preferred_element_type=jnp.float32
            ).astype(jnp.bfloat16)

            @pl.when(mask == 0)
            def _():
                returned[pool * 4, :, cols] = result

            @pl.when(mask != 0)
            def _():
                hidden_out[slot_group, :, cols] = result

            @pl.when((mask != 0) & (slot_group >= 4))
            def _():
                back_copy(slot_group, part).start()

    def back_arrival(pool, mask, part):
        return remote(
            hidden_out.at[0, :, part_cols(part)],
            returned.at[pool * 4 + mask, :, part_cols(part)],
            back_send.at[0],
            back_recv.at[(pool * 4 + mask) * COLUMN_PARTS + part],
            partner,
        )

    def combined(pool, part):
        acc = None
        for mask in range(4):
            if mask:
                with jax.named_scope("k_back_wait"):
                    back_arrival(pool, mask, part).wait_recv()
            in_a, in_b = slot_rows(pool, mask)
            weight = jnp.where(in_a, pool_info[pool, top_count : top_count + 1, :], 0.0)
            weight += jnp.where(in_b, pool_info[pool, top_count + 1 : top_count + 2, :], 0.0)
            high = weight.astype(jnp.bfloat16)
            low = (weight - high.astype(jnp.float32)).astype(jnp.bfloat16)
            values = returned[pool * 4 + mask, :, part_cols(part)]
            for term in (high, low):
                product = lax.dot_general(
                    term, values, (((0,), (0,)), ((), ())), preferred_element_type=jnp.float32
                )
                acc = product if acc is None else acc + product
        return acc

    def sum_copy(chunk, part):
        return remote(
            sum_out.at[chunk, :, part_cols(part)],
            sum_in.at[:, part_cols(part)],
            sum_send.at[chunk * COLUMN_PARTS + part],
            sum_recv.at[part],
            at_chip(jnp.where(chunk == 0, far_outer, far_inner)),
        )

    def return_sums(chunk, part):
        sum_out[chunk, :, part_cols(part)] = combined(1 + chunk, part).astype(jnp.bfloat16)
        sum_copy(chunk, part).start()

    def pick_entry(turn, inner_list, outer_list):
        value = jnp.int32(0)
        for at, (one, two) in enumerate(zip(inner_list, outer_list)):
            value = jnp.where(turn == at, jnp.where(inner, one, two), value)
        return value

    @pl.loop(0, len(INNER_TURNS))
    def _(turn):
        @pl.when(inner & ((turn == 1) | (turn == 3)))
        def _():
            relay(turn // 2)

        @pl.when(inner & (turn == 1))
        def _():
            send_own(3)

        @pl.when(inner & (turn >= 4))
        def _():
            return_sums(turn // 2 - 2, turn % 2)

        @pl.when(turn == 4)
        def _():
            flag_recv[0] = flag_send[...]

            @pl.loop(1, chips)
            def _(offset):
                flag_copy(offset).start()

        amount = pick_entry(turn, [len(t) for t in INNER_TURNS], [len(t) for t in OUTER_TURNS])
        first = pick_entry(
            turn, [(t + (0,))[0] for t in INNER_TURNS], [(t + (0,))[0] for t in OUTER_TURNS]
        )
        second = pick_entry(
            turn, [(t + (0, 0))[1] for t in INNER_TURNS], [(t + (0, 0))[1] for t in OUTER_TURNS]
        )

        @pl.loop(0, amount)
        def _(which):
            first_half(jnp.where(which == 0, first, second))

        @pl.loop(0, amount)
        def _(which):
            second_half(jnp.where(which == 0, first, second))

        @pl.when(turn == 5)
        def _():
            @pl.loop(1, 4)
            def _(mask):
                for part in range(COLUMN_PARTS):
                    back_copy(mask, part).start()

    @pl.loop(1, chips)
    def _(offset):
        flag_copy(offset).wait()

    flag_far[0] = jnp.max(flag_recv[...], axis=0)
    far_copies = [
        remote(
            flag_far.at[0],
            flag_far.at[far],
            far_ssem.at[far],
            far_rsem.at[far],
            {"groups": lax.rem(group + far, groups)},
        )
        for far in range(1, groups)
    ]
    for copy in far_copies:
        copy.start()

    @pl.loop(0, COLUMN_PARTS)
    def _(part):
        total[:, part_cols(part)] = combined(0, part)

    def out_cols(part):
        return pl.ds(pl.multiple_of(core * half + part * piece, 128), piece)

    def own_out(part):
        return pltpu.make_async_copy(
            mixed.at[my_rows, part_cols(part)],
            out.at[:, out_cols(part)],
            out_sem.at[part],
        )

    def pair_out(part):
        return remote(
            mixed.at[your_rows, part_cols(part)],
            out.at[:, out_cols(part)],
            out_send.at[part],
            out_recv.at[part],
            partner,
        )

    for part in range(COLUMN_PARTS):
        cols = slice(part * piece, (part + 1) * piece)
        with jax.named_scope("k_sum_wait"):
            remote(
                sum_out.at[0, :, cols],
                sum_in.at[:, cols],
                sum_send.at[0],
                sum_recv.at[part],
                partner,
            ).wait_recv()
        mixed[:, cols] = (total[:, cols] + sum_in[:, cols].astype(jnp.float32)).astype(
            jnp.bfloat16
        )
        pair_out(part).start()
        own_out(part).start()

    for copy in far_copies:
        copy.wait()
    flag_out[0] = jnp.max(flag_far[...]).astype(jnp.int32)

    for target in range(cores):
        far_info(target).wait_send()

    for part in range(COLUMN_PARTS):
        for target in range(cores):
            far_copy(part, target).wait_send()

    @pl.loop(1, 4)
    def _(mask):
        own_row_copy(mask).wait_send()

    @pl.loop(0, 8)
    def _(slot_group):
        _, mask = home_of(slot_group)

        @pl.when(mask != 0)
        def _():
            for part in range(COLUMN_PARTS):
                back_copy(slot_group, part).wait_send()

    @pl.when(inner)
    def _():
        @pl.loop(0, FAR_CHUNKS * COLUMN_PARTS)
        def _(step):
            chunk = step // COLUMN_PARTS
            part = step % COLUMN_PARTS
            sum_copy(chunk, part).wait_send()

            @pl.loop(1, 4)
            def _(mask):
                relay_copy(chunk, mask, part).wait_send()

    for part in range(COLUMN_PARTS):
        own_out(part).wait()
        pair_out(part).wait()


def two_level_call(slots, tok_rows, half, hidden_size, groups, weight_shapes):
    cores = SPLIT
    chips = lax.axis_size("ep") // cores
    pooled = cores * tok_rows
    dma = pltpu.SemaphoreType.DMA
    pieces = FAR_CHUNKS * COLUMN_PARTS
    any_space = pl.BlockSpec(memory_space=pl.ANY)
    vmem_space = pl.BlockSpec(memory_space=pltpu.VMEM)
    smem_space = pl.BlockSpec(memory_space=pltpu.SMEM)
    bf16, f32 = jnp.bfloat16, jnp.float32
    return pl.pallas_call(
        functools.partial(two_level_kernel, groups, slots),
        out_shape=(
            jax.ShapeDtypeStruct((tok_rows, cores * half), bf16),
            jax.ShapeDtypeStruct((1,), jnp.int32),
        ),
        in_specs=[any_space] + [vmem_space] * 3 + [smem_space] + [any_space] * 3 + [smem_space] * 3,
        out_specs=(any_space, smem_space),
        scratch_shapes=[
            pltpu.VMEM((pooled, half), bf16),
            pltpu.VMEM((FAR_CHUNKS, pooled, half), bf16),
            pltpu.VMEM((3 * cores, 8, tok_rows), f32),
            pltpu.VMEM((3, 8, pooled), f32),
            pltpu.VMEM((3, 2 * chips, pooled), f32),
            pltpu.VMEM(weight_shapes[0], bf16),
            pltpu.VMEM(weight_shapes[1], bf16),
            pltpu.VMEM(weight_shapes[2], bf16),
            pltpu.VMEM((12, slots, half), bf16),
            pltpu.VMEM((8, slots, half), bf16),
            pltpu.VMEM((8, slots, 2 * hidden_size), bf16),
            pltpu.VMEM((8, slots, 2 * hidden_size), bf16),
            pltpu.VMEM((8, slots, half), bf16),
            pltpu.VMEM((12, slots, half), bf16),
            pltpu.VMEM((FAR_CHUNKS, pooled, half), bf16),
            pltpu.VMEM((pooled, half), bf16),
            pltpu.VMEM((pooled, half), f32),
            pltpu.VMEM((pooled, half), bf16),
            pltpu.VMEM((8, 128), f32),
            pltpu.VMEM((chips, 8, 128), f32),
            pltpu.VMEM((groups, 8, 128), f32),
            dma((1,)),
            dma((3,)),
            dma((2,)),
            dma((2,)),
            dma((cores,)),
            dma((2 * cores,)),
            dma((COLUMN_PARTS * cores,)),
            dma((pieces * cores,)),
            dma((12 * COLUMN_PARTS,)),
            dma((8 * COLUMN_PARTS,)),
            dma((8,)),
            dma((8,)),
            dma((8 * COLUMN_PARTS,)),
            dma((12 * COLUMN_PARTS,)),
            dma((pieces,)),
            dma((COLUMN_PARTS,)),
            dma((COLUMN_PARTS,)),
            dma((COLUMN_PARTS,)),
            dma((COLUMN_PARTS,)),
            dma((chips,)),
            dma((chips,)),
            dma((groups,)),
            dma((groups,)),
        ],
        compiler_params=pltpu.CompilerParams(
            collective_id=0, has_side_effects=True, vmem_limit_bytes=62 * 1024 * 1024
        ),
    )


def direct_call(chips, slots, tok_rows, half, hidden_size, groups, weight_shapes):
    cores = SPLIT
    width = cores * half
    pooled = cores * tok_rows
    any_space = pl.BlockSpec(memory_space=pl.ANY)
    vmem_space = pl.BlockSpec(memory_space=pltpu.VMEM)
    smem_space = pl.BlockSpec(memory_space=pltpu.SMEM)
    dma = pltpu.SemaphoreType.DMA
    return pl.pallas_call(
        functools.partial(fused_kernel, chips, cores, groups, slots),
        out_shape=(
            jax.ShapeDtypeStruct((tok_rows, width), jnp.bfloat16),
            jax.ShapeDtypeStruct((1,), jnp.int32),
        ),
        in_specs=[any_space] + [vmem_space] * 3 + [smem_space] + [any_space] * 3 + [smem_space] * 3,
        out_specs=(any_space, smem_space),
        scratch_shapes=[
            pltpu.VMEM((pooled, half), jnp.bfloat16),
            pltpu.VMEM((cores, 8, tok_rows), jnp.float32),
            pltpu.VMEM((pooled, 8), jnp.float32),
            pltpu.VMEM(weight_shapes[0], jnp.bfloat16),
            pltpu.VMEM(weight_shapes[1], jnp.bfloat16),
            pltpu.VMEM(weight_shapes[2], jnp.bfloat16),
            pltpu.VMEM((pooled, 128), jnp.float32),
            pltpu.VMEM((pooled, 128), jnp.float32),
            pltpu.VMEM((chips, slots, half), jnp.bfloat16),
            pltpu.VMEM((chips, slots, half), jnp.bfloat16),
            pltpu.VMEM((chips, slots, 2 * hidden_size), jnp.bfloat16),
            pltpu.VMEM((chips, slots, 2 * hidden_size), jnp.bfloat16),
            pltpu.VMEM((chips, slots, half), jnp.bfloat16),
            pltpu.VMEM((chips, slots, half), jnp.bfloat16),
            pltpu.VMEM((pooled, half), jnp.float32),
            pltpu.VMEM((pooled, half), jnp.bfloat16),
            pltpu.VMEM((8, 128), jnp.float32),
            pltpu.VMEM((chips, 8, 128), jnp.float32),
            pltpu.VMEM((groups, 8, 128), jnp.float32),
            dma((3,)),
            dma((3,)),
            dma((3,)),
            dma((3,)),
            dma((chips,)),
            dma((chips,)),
            dma((chips,)),
            dma((chips,)),
            dma((chips,)),
            dma((chips,)),
            dma((chips,)),
            dma((chips,)),
            dma((groups,)),
            dma((groups,)),
        ],
        compiler_params=pltpu.CompilerParams(
            collective_id=0, has_side_effects=True, vmem_limit_bytes=60 * 1024 * 1024
        ),
    )


def two_level_fits(chips, tok_rows, half):
    return chips == 8 and tok_rows == 128 and half % (128 * COLUMN_PARTS) == 0


def per_device(
    tokens, host, copy, gate_prob, hot, w_gate, w_up, w_down, gate_scale, up_scale, down_scale
):
    cores = SPLIT
    chips = lax.axis_size("ep") // cores
    groups = lax.axis_size("groups")
    tok_rows, width = tokens.shape
    half = width // cores
    hidden_size = w_gate.shape[2]
    pooled = cores * tok_rows
    slots = pooled_slots(pooled, host.shape[1], chips)
    args = (
        tokens,
        host.T,
        copy.T,
        gate_prob.T,
        hot,
        w_gate,
        w_up,
        w_down,
        gate_scale[0].T,
        up_scale[0].T,
        down_scale[0],
    )
    weight_shapes = (w_gate.shape[1:], w_up.shape[1:], w_down.shape[1:])
    if two_level_fits(chips, tok_rows, half):
        call = two_level_call(slots, tok_rows, half, hidden_size, groups, weight_shapes)
    else:
        call = direct_call(chips, slots, tok_rows, half, hidden_size, groups, weight_shapes)
    out, flag = call(*args)
    return lax.cond(
        flag[0] > 0,
        lambda: padded_exchange(
            tokens,
            host,
            copy,
            gate_prob,
            hot,
            w_gate,
            w_up,
            w_down,
            gate_scale,
            up_scale,
            down_scale,
        ),
        lambda: out,
    )


def solution(mesh):
    return jax.shard_map(
        per_device,
        mesh=mesh,
        in_specs=(
            P(("groups", "ep"), None),
            P(("groups", "ep"), None),
            P(("groups", "ep"), None),
            P(("groups", "ep"), None),
            P(),
            P("ep", None, None),
            P("ep", None, None),
            P("ep", None, None),
            P("ep", None, None),
            P("ep", None, None),
            P("ep", None, None),
        ),
        out_specs=P(("groups", "ep"), None),
        check_vma=False,
    )
```
